32 devices in a mesh: rows: 8 (over z, x), grp: 4 (over y, core).
Axes of the slice: x: 2, y: 2, z: 4, core: 2. Of those that a mesh axis runs over, the one named last changes fastest.
Arguments:
- matrix: float32 [65536, 1024], P(('rows', 'grp'))
- row_signs: int32 [65536], P(('rows', 'grp')), may hold values from -1 to 1, as said below
- samples: int32 [8192], P(('rows', 'grp')), may hold values from 0 to 65535, as said below
Outputs:
- factor: float32 [1024, 1024], P('rows')
The draws below stay inside these ranges and needn't reach their ends.
Inputs may be any that keep to these rules, and one draw needn't show every extreme that they name: `row_signs`: every entry is 1 or -1. `samples`: entries are distinct and increasing; entries k * 256 to (k + 1) * 256 - 1 lie in rows k * 2048 to (k + 1) * 2048 - 1.
All inputs are finite; a program needn't handle non-finite values.
Results may differ from the reference program's by a relative error of at most 0.00011.
Values sent between devices are 32-bit elements; how exact they have to be, the bound alone decides.
A program may use at most 128 MiB of HBM per device.

```python
import jax
import jax.numpy as jnp
from jax import lax

COLS = 1024
ROW_DEV = 2048
SAMPLES = 8192
ROWS_TOTAL = 65536


def draw_matrix(key, part):
    key_noise = jax.random.fold_in(key, 11)
    key_common = jax.random.fold_in(key, 12)
    key_cols = jax.random.fold_in(key, 13)
    col_scale = jnp.exp(jax.random.uniform(key_cols, (COLS,), jnp.float32, jnp.log(0.5), jnp.log(4.0)))
    noise = jax.random.normal(key_noise, (ROWS_TOTAL, COLS), jnp.float32)
    common = jax.random.normal(key_common, (ROWS_TOTAL, 1), jnp.float32)
    mixed_rows = noise + 0.5 * jnp.roll(noise, 1, axis=1) + 0.6 * common
    return (mixed_rows * col_scale[None, :] / jnp.sqrt(jnp.float32(ROWS_TOTAL))).astype(jnp.float32)


def draw_row_signs(key, part):
    coin_key = jax.random.fold_in(key, 21)
    return (2 * jax.random.randint(coin_key, (ROWS_TOTAL,), 0, 2) - 1).astype(jnp.int32)


def draw_samples(key, part):
    pick_key = jax.random.fold_in(key, 31)
    block_count = ROWS_TOTAL // ROW_DEV
    per_block = SAMPLES // block_count
    block_keys = jax.random.split(pick_key, block_count)
    picks = jax.vmap(lambda one_key: jnp.sort(jax.random.permutation(one_key, ROW_DEV)[:per_block]))(block_keys)
    offsets = ROW_DEV * jnp.arange(block_count, dtype=jnp.int32)[:, None]
    return (picks.astype(jnp.int32) + offsets).reshape(block_count * per_block).astype(jnp.int32)


def setup_inputs(seed: int = 0) -> dict:
    keys = jax.random.split(jax.random.key(seed), 4)
    return {
        "matrix": draw_matrix(jax.random.fold_in(keys[3], 71), 0),
        "row_signs": draw_row_signs(jax.random.fold_in(keys[3], 71), 0),
        "samples": draw_samples(jax.random.fold_in(keys[3], 71), 0),
    }


def walsh_transform(values):
    length, width_cols = values.shape
    half_span = 1
    for section_level in range(length.bit_length() - 1):
        paired = values.reshape(length // (2 * half_span), 2, half_span, width_cols)
        values = jnp.stack([paired[:, 0] + paired[:, 1], paired[:, 0] - paired[:, 1]], axis=1).reshape(length, width_cols)
        half_span = half_span * 2
    return values

def reference(matrix, row_signs, samples):
    total_rows = matrix.shape[0]
    signed = matrix * row_signs.astype(jnp.float32)[:, None]
    transformed = walsh_transform(signed) / jnp.sqrt(jnp.float32(total_rows))
    sampled = transformed[samples] * jnp.sqrt(jnp.float32(total_rows / SAMPLES))
    gram_total = jnp.dot(sampled.T, sampled, precision=lax.Precision.HIGHEST)
    lower_factor = jnp.linalg.cholesky(gram_total)
    return lower_factor.T
```

```python
import functools

import jax
import jax.numpy as jnp
from jax import lax
from jax.experimental import pallas as pl
from jax.experimental.pallas import tpu as pltpu
from jax.sharding import PartitionSpec as P

MESH = pl.DeviceIdType.MESH
VMEM_LIMIT = 60 * 1024 * 1024
TILE = 128


def sylvester(length):
    matrix = jnp.ones((1, 1), jnp.float32)
    while matrix.shape[0] < length:
        matrix = jnp.block([[matrix, matrix], [matrix, -matrix]])
    return matrix


def butterfly(parts):
    span = 1
    while span < len(parts):
        parts = list(parts)
        for start in range(0, len(parts), 2 * span):
            for i in range(start, start + span):
                low, high = parts[i], parts[i + span]
                parts[i], parts[i + span] = low + high, low - high
        span *= 2
    return parts


def split(x):
    high = x.astype(jnp.bfloat16)
    return high, (x - high.astype(jnp.float32)).astype(jnp.bfloat16)


def local_kernel(base, x_ref, s_ref, h_ref, o_ref):
    parts = []
    for i in range(x_ref.shape[0] // base):
        rows = slice(i * base, (i + 1) * base)
        high, low = split(x_ref[rows, :] * s_ref[rows, :])
        both = jnp.dot(h_ref[...], high, preferred_element_type=jnp.float32)
        both += jnp.dot(h_ref[...], low, preferred_element_type=jnp.float32)
        parts.append(both)
    for i, part in enumerate(butterfly(parts)):
        o_ref[i * base : (i + 1) * base, :] = part


def local_transform(matrix, signs, base):
    rows, cols = matrix.shape
    return pl.pallas_call(
        functools.partial(local_kernel, base),
        grid=(cols // TILE,),
        out_shape=jax.ShapeDtypeStruct((rows, cols), jnp.float32),
        in_specs=[
            pl.BlockSpec((rows, TILE), lambda c: (0, c)),
            pl.BlockSpec((rows, TILE), lambda c: (0, 0)),
            pl.BlockSpec((base, base), lambda c: (0, 0)),
        ],
        out_specs=pl.BlockSpec((rows, TILE), lambda c: (0, c)),
        compiler_params=pltpu.CompilerParams(vmem_limit_bytes=VMEM_LIMIT),
    )(matrix, signs, sylvester(base).astype(jnp.bfloat16))


def gram_kernel(scale, x_ref, w_ref, o_ref, left, right):
    blocks, step, cols = x_ref.shape
    rows = blocks * step

    @pl.when(pl.program_id(0) == 0)
    def _():
        o_ref[...] = jnp.zeros_like(o_ref)

    def mix(c, carry):
        at = pl.ds(pl.multiple_of(c * TILE, TILE), TILE)
        parts = butterfly([x_ref[b, :, at] for b in range(blocks)])
        for b in range(0, blocks, 2):
            x = jnp.concatenate(parts[b : b + 2], axis=0) * scale
            w = jnp.concatenate([w_ref[b], w_ref[b + 1]], axis=0)
            high, low = split(x)
            here = slice(b * step, (b + 2) * step)
            there = slice(rows + b * step, rows + (b + 2) * step)
            masked = (high.astype(jnp.float32) * w).astype(jnp.bfloat16)
            left[here, at] = masked
            right[here, at] = high
            left[there, at] = masked
            right[there, at] = (2.0 * low.astype(jnp.float32)).astype(jnp.bfloat16)
        return carry

    lax.fori_loop(0, cols // TILE, mix, 0)
    wide = 2 * TILE

    def add(n, carry):
        at = pl.ds(pl.multiple_of(n * wide, wide), wide)
        o_ref[:, at] += lax.dot_general(
            left[...], right[:, at], (((0,), (0,)), ((), ())), preferred_element_type=jnp.float32
        )
        return carry

    lax.fori_loop(0, cols // wide, add, 0)


def gram_share(arrived, weights, scale):
    blocks, piece, cols = arrived.shape
    step = 8
    return pl.pallas_call(
        functools.partial(gram_kernel, scale),
        grid=(piece // step,),
        out_shape=jax.ShapeDtypeStruct((cols, cols), jnp.float32),
        in_specs=[
            pl.BlockSpec((blocks, step, cols), lambda t: (0, t, 0)),
            pl.BlockSpec((blocks, step, TILE), lambda t: (0, t, 0)),
        ],
        out_specs=pl.BlockSpec((cols, cols), lambda t: (0, 0)),
        scratch_shapes=[pltpu.VMEM((2 * blocks * step, cols), jnp.bfloat16)] * 2,
        compiler_params=pltpu.CompilerParams(vmem_limit_bytes=VMEM_LIMIT),
    )(arrived, weights)


def panel_tiles(panels):
    sizes = [panels - i + (panels - i) % 2 for i in range(panels)]
    return sizes, [sum(sizes[:i]) for i in range(panels)]


def segments(panels):
    sizes, starts = panel_tiles(panels)
    runs = [(0, 1), (1, 2), (2, 4), (4, panels)]
    return [(starts[i], sum(sizes[i:j])) for i, j in runs]


def dot3(a, b, dims):
    (ah, al), (bh, bl) = a, b
    go = functools.partial(lax.dot_general, dimension_numbers=(dims, ((), ())), preferred_element_type=jnp.float32)
    return go(ah, bh) + (go(ah, bl) + go(al, bh))

def spread(row):
    return jnp.broadcast_to(row, (8, TILE))

def factor_block(block, lines):
    count, group = TILE // 8, 4
    sub_id = lax.broadcasted_iota(jnp.int32, (8, TILE), 0)
    lane_id = lax.broadcasted_iota(jnp.int32, (8, TILE), 1)
    strips = [block[8 * i : 8 * i + 8, :] for i in range(count)]
    inverse = [(lane_id == sub_id + 8 * i).astype(jnp.float32) for i in range(count)]
    for first in range(0, count, group):
        last = first + group
        for s in range(first, last):
            columns = {
                i: [jnp.broadcast_to(strips[i][:, 8 * s + t : 8 * s + t + 1], (8, TILE)) for t in range(8)]
                for i in range(s, last)
            }
            for t in range(8):
                lines[s % 2, t] = columns[s][t]
            lines[s % 2, 8] = strips[s]
            lines[s % 2, 9] = inverse[s]
            pivot = {(r, t): spread(lines[s % 2, t, r : r + 1, :]) for t in range(8) for r in range(t, 8)}
            row = [spread(lines[s % 2, 8, q : q + 1, :]) for q in range(8)]
            inv_row = [spread(lines[s % 2, 9, q : q + 1, :]) for q in range(8)]
            for j in range(8):
                root = lax.rsqrt(pivot[j, j])
                for r in range(j + 1, 8):
                    pivot[r, j] = pivot[r, j] * root
                for t in range(j + 1, 8):
                    for r in range(t, 8):
                        pivot[r, t] = pivot[r, t] - pivot[r, j] * pivot[t, j]
                row[j] = row[j] * root
                inv_row[j] = inv_row[j] * root
                for r in range(j + 1, 8):
                    row[r] = row[r] - pivot[r, j] * row[j]
                    inv_row[r] = inv_row[r] - pivot[r, j] * inv_row[j]
                for i in range(s + 1, last):
                    left = columns[i]
                    left[j] = left[j] * root
                    for r in range(j + 1, 8):
                        left[r] = left[r] - pivot[r, j] * left[j]
                    strips[i] = strips[i] - left[j] * row[j]
                    inverse[i] = inverse[i] - left[j] * inv_row[j]
            for q in range(8):
                strips[s] = row[q] if q == 0 else jnp.where(sub_id == q, row[q], strips[s])
                inverse[s] = inv_row[q] if q == 0 else jnp.where(sub_id == q, inv_row[q], inverse[s])
        if last < count:
            high, low = split(jnp.concatenate(strips[first:last], axis=0))
            inv_high, inv_low = split(jnp.concatenate(inverse[first:last], axis=0))
            three = jnp.concatenate([high, low, high], axis=0)
            rest = jnp.concatenate([high, high, low], axis=0)
            inv_rest = jnp.concatenate([inv_high, inv_high, inv_low], axis=0)
            both = jnp.concatenate([rest, inv_rest], axis=1)
            change = lax.dot_general(three, both, (((0,), (0,)), ((), ())), preferred_element_type=jnp.float32)
            for i in range(last, count):
                strips[i] = strips[i] - change[8 * i : 8 * i + 8, :TILE]
                inverse[i] = inverse[i] - change[8 * i : 8 * i + 8, TILE:]
    return jnp.concatenate(inverse, axis=0)


def factor_panels(work, u_ref, lines, high, low):
    cols = u_ref.shape[0]

    def panel(k, carry):
        base = pl.multiple_of(k * TILE, TILE)
        here = pl.ds(base, TILE)
        lower = split(factor_block(work[here, here], lines))
        wide_row = lax.broadcasted_iota(jnp.int32, (TILE, cols), 0) + base
        wide_lane = lax.broadcasted_iota(jnp.int32, (TILE, cols), 1)
        upper = dot3(lower, split(work[here, :]), ((1,), (0,)))
        upper = jnp.where(wide_lane >= wide_row, upper, 0.0)
        u_ref[here, :] = upper
        high[...], low[...] = split(upper)

        def trail(start, i, inner):
            there = pl.ds(pl.multiple_of(i * TILE, TILE), TILE)
            right = (high[:, start:], low[:, start:])
            work[there, start:] -= dot3((high[:, there], low[:, there]), right, ((0,), (0,)))
            return inner

        half = cols // TILE // 2
        lax.fori_loop(k + 1, half, functools.partial(trail, 0), 0)
        lax.fori_loop(jnp.maximum(k + 1, half), cols // TILE, functools.partial(trail, cols // 2), 0)
        return carry

    lax.fori_loop(0, cols // TILE, panel, 0)


def unpack(source, work, panels):
    for i, start in enumerate(panel_tiles(panels)[1]):
        for j in range(i, panels):
            p = (start + j - i) * TILE
            work[i * TILE : (i + 1) * TILE, j * TILE : (j + 1) * TILE] = source[p : p + TILE, :]


def factor_kernel(g_ref, u_ref, work, lines, high, low):
    work[...] = jnp.zeros_like(work)
    unpack(g_ref, work, u_ref.shape[0] // TILE)
    factor_panels(work, u_ref, lines, high, low)


def reduce_factor_kernel(
    groups, g_ref, u_ref, whole, in1, in2, in3, sum1, sum2, send, arrive, work, lines, high, low
):
    pair, plane, line = groups
    width = lax.axis_size("grp")
    me = lax.axis_index("rows") * width + lax.axis_index("grp")
    c, q, b = me % pair, (me // pair) % plane, me // (pair * plane)

    def at(cc, qq, bb):
        index = (bb * plane + qq) * pair + cc
        return (index // width, index % width)

    peers = [at((c + t) % pair, q, b) for t in range(1, pair)]
    peers += [at(c, (q + t) % plane, b) for t in range(1, plane)]
    peers += [at(c, q, (b + t) % line) for t in range(1, line)]
    barrier = pltpu.get_barrier_semaphore()
    for peer in peers:
        pl.semaphore_signal(barrier, inc=1, device_id=peer, device_id_type=MESH)
    pl.semaphore_wait(barrier, len(peers))

    runs = segments(u_ref.shape[0] // TILE)
    copies = {}

    def start(s, stage, t, source, target, peer):
        slot = stage * 4 + t
        copy = pltpu.make_async_remote_copy(
            src_ref=source,
            dst_ref=target,
            send_sem=send.at[s, slot],
            recv_sem=arrive.at[s, slot],
            device_id=peer,
            device_id_type=MESH,
        )
        copy.start()
        copies[s, stage, t] = copy

    def rows(first, count):
        return pl.ds(pl.multiple_of(first, 8), count)

    def sizes(s):
        first, tiles = runs[s]
        first, n1 = first * TILE, tiles * TILE
        return first, n1 // pair, n1 // (pair * plane), n1 // (pair * plane * line)

    def scatter1(s):
        first, n1, n2, n3 = sizes(s)
        for t in range(1, pair):
            other = (c + t) % pair
            start(s, 0, t, g_ref.at[rows(first + other * n1, n1)], in1.at[t - 1, rows(first // pair, n1)], at(other, q, b))

    def scatter2(s):
        first, n1, n2, n3 = sizes(s)
        mine = rows(first // pair, n1)
        total = g_ref[rows(first + c * n1, n1), :]
        for t in range(1, pair):
            copies[s, 0, t].wait_recv()
            total = total + in1[t - 1, mine, :]
        sum1[mine, :] = total
        for t in range(1, plane):
            other = (q + t) % plane
            start(s, 1, t, sum1.at[rows(first // pair + other * n2, n2)], in2.at[t - 1, rows(first // (pair * plane), n2)], at(c, other, b))

    def scatter3(s):
        first, n1, n2, n3 = sizes(s)
        mine = rows(first // (pair * plane), n2)
        total = sum1[rows(first // pair + q * n2, n2), :]
        for t in range(1, plane):
            copies[s, 1, t].wait_recv()
            total = total + in2[t - 1, mine, :]
        sum2[mine, :] = total
        for t in range(1, line):
            other = (b + t) % line
            start(s, 2, t, sum2.at[rows(first // (pair * plane) + other * n3, n3)], in3.at[t - 1, rows(first // (pair * plane * line), n3)], at(c, q, other))

    def gather3(s):
        first, n1, n2, n3 = sizes(s)
        mine = rows(first // (pair * plane * line), n3)
        total = sum2[rows(first // (pair * plane) + b * n3, n3), :]
        for t in range(1, line):
            copies[s, 2, t].wait_recv()
            total = total + in3[t - 1, mine, :]
        here = rows(first + c * n1 + q * n2 + b * n3, n3)
        whole[here, :] = total
        for t in range(1, line):
            start(s, 3, t, whole.at[here], whole.at[here], at(c, q, (b + t) % line))

    def gather2(s):
        first, n1, n2, n3 = sizes(s)
        for t in range(1, line):
            copies[s, 3, t].wait_recv()
        here = rows(first + c * n1 + q * n2, n2)
        for t in range(1, plane):
            start(s, 4, t, whole.at[here], whole.at[here], at(c, (q + t) % plane, b))

    def gather1(s):
        first, n1, n2, n3 = sizes(s)
        for t in range(1, plane):
            copies[s, 4, t].wait_recv()
        here = rows(first + c * n1, n1)
        for t in range(1, pair):
            start(s, 5, t, whole.at[here], whole.at[here], at((c + t) % pair, q, b))

    def finish(s):
        for t in range(1, pair):
            copies[s, 5, t].wait_recv()

    stages = [scatter1, scatter2, scatter3, gather3, gather2, gather1, finish]
    for step in range(len(runs) + len(stages) - 1):
        for k in reversed(range(len(stages))):
            if 0 <= step - k < len(runs):
                stages[k](step - k)
    for copy in copies.values():
        copy.wait_send()
    unpack(whole, work, u_ref.shape[0] // TILE)
    factor_panels(work, u_ref, lines, high, low)


def reduce_factor(packed, cols):
    devices = lax.axis_size("rows") * lax.axis_size("grp")
    rows = packed.shape[0]
    common = [
        pltpu.VMEM((cols, cols), jnp.float32),
        pltpu.VMEM((2, 10, 8, TILE), jnp.float32),
        pltpu.VMEM((TILE, cols), jnp.bfloat16),
        pltpu.VMEM((TILE, cols), jnp.bfloat16),
    ]
    call = functools.partial(
        pl.pallas_call,
        out_shape=jax.ShapeDtypeStruct((cols, cols), jnp.float32),
        in_specs=[pl.BlockSpec(memory_space=pltpu.VMEM)],
        out_specs=pl.BlockSpec(memory_space=pltpu.VMEM),
    )
    pair, plane = 2, 4
    line = devices // (pair * plane)
    if devices % (pair * plane) or line > 4 or any(tiles * TILE % (8 * devices) for _, tiles in segments(cols // TILE)):
        return call(
            factor_kernel,
            scratch_shapes=common,
            compiler_params=pltpu.CompilerParams(vmem_limit_bytes=VMEM_LIMIT),
        )(lax.psum(packed, ("rows", "grp")))
    runs = len(segments(cols // TILE))
    return call(
        functools.partial(reduce_factor_kernel, (pair, plane, line)),
        scratch_shapes=[
            pltpu.VMEM((rows, TILE), jnp.float32),
            pltpu.VMEM((pair - 1, rows // pair, TILE), jnp.float32),
            pltpu.VMEM((plane - 1, rows // (pair * plane), TILE), jnp.float32),
            pltpu.VMEM((max(line - 1, 1), rows // devices, TILE), jnp.float32),
            pltpu.VMEM((rows // pair, TILE), jnp.float32),
            pltpu.VMEM((rows // (pair * plane), TILE), jnp.float32),
            pltpu.SemaphoreType.DMA((runs, 24)),
            pltpu.SemaphoreType.DMA((runs, 24)),
            *common,
        ],
        compiler_params=pltpu.CompilerParams(vmem_limit_bytes=VMEM_LIMIT, collective_id=1, has_side_effects=True),
    )(packed)


def shards(matrix, row_signs, samples):
    count_rows = lax.axis_size("rows")
    blocks = count_rows * lax.axis_size("grp")
    row_dev, col_count = matrix.shape
    piece_rows = row_dev // blocks
    sample_dev = samples.shape[0]
    position = lax.axis_index(("rows", "grp"))
    all_indices = lax.all_gather(samples, ("rows", "grp"), axis=0)
    signs = jnp.broadcast_to(row_signs.astype(jnp.float32)[:, None], (row_dev, TILE))
    before = local_transform(matrix, signs, min(256, row_dev))
    arrived = lax.all_to_all(
        before.reshape(blocks, piece_rows, col_count),
        ("rows", "grp"),
        split_axis=0,
        concat_axis=0,
        tiled=True,
    )
    first = jnp.arange(blocks, dtype=jnp.int32)[:, None] * row_dev + position * piece_rows
    within = all_indices - first
    hits = within[:, None, :] == jnp.arange(piece_rows, dtype=jnp.int32)[None, :, None]
    weights = jnp.max(hits.astype(jnp.float32), axis=2)
    weights = jnp.broadcast_to(weights[:, :, None], (blocks, piece_rows, TILE))
    scale = (sample_dev * blocks) ** -0.5
    half = gram_share(arrived, weights, scale)
    whole = (half + half.T) * 0.5
    pieces = []
    for i, count in enumerate(panel_tiles(col_count // TILE)[0]):
        row = whole[i * TILE : (i + 1) * TILE]
        tiles = [row[:, j * TILE : (j + 1) * TILE] for j in range(i, col_count // TILE)]
        tiles += [jnp.zeros((TILE, TILE), jnp.float32)] * (count - len(tiles))
        pieces += tiles
    upper_factor = reduce_factor(jnp.concatenate(pieces, axis=0), col_count)
    share_rows = col_count // count_rows
    return lax.dynamic_slice_in_dim(
        upper_factor, lax.axis_index("rows") * share_rows, share_rows, 0
    )


def solution(mesh):
    return jax.shard_map(
        shards,
        mesh=mesh,
        in_specs=(P(("rows", "grp"), None), P(("rows", "grp")), P(("rows", "grp"))),
        out_specs=P("rows", None),
        check_vma=False,
    )
```

```python
import functools

import jax
import jax.numpy as jnp
from jax import lax
from jax.experimental import pallas as pl
from jax.experimental.pallas import tpu as pltpu
from jax.sharding import PartitionSpec as P

MESH = pl.DeviceIdType.MESH
VMEM_LIMIT = 60 * 1024 * 1024
TILE = 128


def sylvester(length):
    matrix = jnp.ones((1, 1), jnp.float32)
    while matrix.shape[0] < length:
        matrix = jnp.block([[matrix, matrix], [matrix, -matrix]])
    return matrix


def butterfly(parts):
    span = 1
    while span < len(parts):
        parts = list(parts)
        for start in range(0, len(parts), 2 * span):
            for i in range(start, start + span):
                low, high = parts[i], parts[i + span]
                parts[i], parts[i + span] = low + high, low - high
        span *= 2
    return parts


def split(x):
    high = x.astype(jnp.bfloat16)
    return high, (x - high.astype(jnp.float32)).astype(jnp.bfloat16)


def local_kernel(base, x_ref, s_ref, h_ref, o_ref):
    parts = []
    for i in range(x_ref.shape[0] // base):
        rows = slice(i * base, (i + 1) * base)
        high, low = split(x_ref[rows, :] * s_ref[rows, :])
        both = jnp.dot(h_ref[...], high, preferred_element_type=jnp.float32)
        both += jnp.dot(h_ref[...], low, preferred_element_type=jnp.float32)
        parts.append(both)
    for i, part in enumerate(butterfly(parts)):
        o_ref[i * base : (i + 1) * base, :] = part


def local_transform(matrix, signs, base):
    rows, cols = matrix.shape
    return pl.pallas_call(
        functools.partial(local_kernel, base),
        grid=(cols // TILE,),
        out_shape=jax.ShapeDtypeStruct((rows, cols), jnp.float32),
        in_specs=[
            pl.BlockSpec((rows, TILE), lambda c: (0, c)),
            pl.BlockSpec((rows, TILE), lambda c: (0, 0)),
            pl.BlockSpec((base, base), lambda c: (0, 0)),
        ],
        out_specs=pl.BlockSpec((rows, TILE), lambda c: (0, c)),
        compiler_params=pltpu.CompilerParams(vmem_limit_bytes=VMEM_LIMIT),
    )(matrix, signs, sylvester(base).astype(jnp.bfloat16))


def gram_kernel(scale, x_ref, w_ref, o_ref, left, right):
    blocks, step, cols = x_ref.shape
    rows = blocks * step

    @pl.when(pl.program_id(0) == 0)
    def _():
        o_ref[...] = jnp.zeros_like(o_ref)

    def mix(c, carry):
        at = pl.ds(pl.multiple_of(c * TILE, TILE), TILE)
        parts = butterfly([x_ref[b, :, at] for b in range(blocks)])
        for b in range(0, blocks, 2):
            x = jnp.concatenate(parts[b : b + 2], axis=0) * scale
            w = jnp.concatenate([w_ref[b], w_ref[b + 1]], axis=0)
            high, low = split(x)
            here = slice(b * step, (b + 2) * step)
            there = slice(rows + b * step, rows + (b + 2) * step)
            masked = (high.astype(jnp.float32) * w).astype(jnp.bfloat16)
            left[here, at] = masked
            right[here, at] = high
            left[there, at] = masked
            right[there, at] = (2.0 * low.astype(jnp.float32)).astype(jnp.bfloat16)
        return carry

    lax.fori_loop(0, cols // TILE, mix, 0)
    wide = 2 * TILE

    def add(n, carry):
        at = pl.ds(pl.multiple_of(n * wide, wide), wide)
        o_ref[:, at] += lax.dot_general(
            left[...], right[:, at], (((0,), (0,)), ((), ())), preferred_element_type=jnp.float32
        )
        return carry

    lax.fori_loop(0, cols // wide, add, 0)


def gram_share(arrived, weights, scale):
    blocks, piece, cols = arrived.shape
    step = 8
    return pl.pallas_call(
        functools.partial(gram_kernel, scale),
        grid=(piece // step,),
        out_shape=jax.ShapeDtypeStruct((cols, cols), jnp.float32),
        in_specs=[
            pl.BlockSpec((blocks, step, cols), lambda t: (0, t, 0)),
            pl.BlockSpec((blocks, step, TILE), lambda t: (0, t, 0)),
        ],
        out_specs=pl.BlockSpec((cols, cols), lambda t: (0, 0)),
        scratch_shapes=[pltpu.VMEM((2 * blocks * step, cols), jnp.bfloat16)] * 2,
        compiler_params=pltpu.CompilerParams(vmem_limit_bytes=VMEM_LIMIT),
    )(arrived, weights)


def panel_tiles(panels):
    sizes = [panels - i + (panels - i) % 2 for i in range(panels)]
    return sizes, [sum(sizes[:i]) for i in range(panels)]


def segments(panels):
    sizes, starts = panel_tiles(panels)
    runs = [(0, 1), (1, 2), (2, 4), (4, panels)]
    return [(starts[i], sum(sizes[i:j])) for i, j in runs]


def dot3(a, b, dims):
    (ah, al), (bh, bl) = a, b
    go = functools.partial(lax.dot_general, dimension_numbers=(dims, ((), ())), preferred_element_type=jnp.float32)
    return go(ah, bh) + (go(ah, bl) + go(al, bh))

def spread(row):
    return jnp.broadcast_to(row, (8, TILE))

def factor_block(block, lines):
    count, group = TILE // 8, 4
    sub_id = lax.broadcasted_iota(jnp.int32, (8, TILE), 0)
    lane_id = lax.broadcasted_iota(jnp.int32, (8, TILE), 1)
    strips = [block[8 * i : 8 * i + 8, :] for i in range(count)]
    inverse = [(lane_id == sub_id + 8 * i).astype(jnp.float32) for i in range(count)]
    for first in range(0, count, group):
        last = first + group
        for s in range(first, last):
            columns = {
                i: [jnp.broadcast_to(strips[i][:, 8 * s + t : 8 * s + t + 1], (8, TILE)) for t in range(8)]
                for i in range(s, last)
            }
            for t in range(8):
                lines[s % 2, t] = columns[s][t]
            lines[s % 2, 8] = strips[s]
            lines[s % 2, 9] = inverse[s]
            pivot = {(r, t): spread(lines[s % 2, t, r : r + 1, :]) for t in range(8) for r in range(t, 8)}
            row = [spread(lines[s % 2, 8, q : q + 1, :]) for q in range(8)]
            inv_row = [spread(lines[s % 2, 9, q : q + 1, :]) for q in range(8)]
            for j in range(8):
                root = lax.rsqrt(pivot[j, j])
                for r in range(j + 1, 8):
                    pivot[r, j] = pivot[r, j] * root
                for t in range(j + 1, 8):
                    for r in range(t, 8):
                        pivot[r, t] = pivot[r, t] - pivot[r, j] * pivot[t, j]
                row[j] = row[j] * root
                inv_row[j] = inv_row[j] * root
                for r in range(j + 1, 8):
                    row[r] = row[r] - pivot[r, j] * row[j]
                    inv_row[r] = inv_row[r] - pivot[r, j] * inv_row[j]
                for i in range(s + 1, last):
                    left = columns[i]
                    left[j] = left[j] * root
                    for r in range(j + 1, 8):
                        left[r] = left[r] - pivot[r, j] * left[j]
                    strips[i] = strips[i] - left[j] * row[j]
                    inverse[i] = inverse[i] - left[j] * inv_row[j]
            for q in range(8):
                strips[s] = row[q] if q == 0 else jnp.where(sub_id == q, row[q], strips[s])
                inverse[s] = inv_row[q] if q == 0 else jnp.where(sub_id == q, inv_row[q], inverse[s])
        if last < count:
            high, low = split(jnp.concatenate(strips[first:last], axis=0))
            inv_high, inv_low = split(jnp.concatenate(inverse[first:last], axis=0))
            three = jnp.concatenate([high, low, high], axis=0)
            rest = jnp.concatenate([high, high, low], axis=0)
            inv_rest = jnp.concatenate([inv_high, inv_high, inv_low], axis=0)
            both = jnp.concatenate([rest, inv_rest], axis=1)
            change = lax.dot_general(three, both, (((0,), (0,)), ((), ())), preferred_element_type=jnp.float32)
            for i in range(last, count):
                strips[i] = strips[i] - change[8 * i : 8 * i + 8, :TILE]
                inverse[i] = inverse[i] - change[8 * i : 8 * i + 8, TILE:]
    return jnp.concatenate(inverse, axis=0)


def factor_panels(work, u_ref, lines, high, low):
    cols = u_ref.shape[0]

    def panel(k, carry):
        base = pl.multiple_of(k * TILE, TILE)
        here = pl.ds(base, TILE)
        lower = split(factor_block(work[here, here], lines))
        wide_row = lax.broadcasted_iota(jnp.int32, (TILE, cols), 0) + base
        wide_lane = lax.broadcasted_iota(jnp.int32, (TILE, cols), 1)
        upper = dot3(lower, split(work[here, :]), ((1,), (0,)))
        upper = jnp.where(wide_lane >= wide_row, upper, 0.0)
        u_ref[here, :] = upper
        high[...], low[...] = split(upper)

        def trail(start, i, inner):
            there = pl.ds(pl.multiple_of(i * TILE, TILE), TILE)
            right = (high[:, start:], low[:, start:])
            work[there, start:] -= dot3((high[:, there], low[:, there]), right, ((0,), (0,)))
            return inner

        half = cols // TILE // 2
        lax.fori_loop(k + 1, half, functools.partial(trail, 0), 0)
        lax.fori_loop(jnp.maximum(k + 1, half), cols // TILE, functools.partial(trail, cols // 2), 0)
        return carry

    lax.fori_loop(0, cols // TILE, panel, 0)


def unpack(source, work, panels):
    for i, start in enumerate(panel_tiles(panels)[1]):
        for j in range(i, panels):
            p = (start + j - i) * TILE
            work[i * TILE : (i + 1) * TILE, j * TILE : (j + 1) * TILE] = source[p : p + TILE, :]


def factor_kernel(g_ref, u_ref, over_ref, work, lines, high, low):
    over_ref[...] = g_ref[g_ref.shape[0] - 8 :, :]
    work[...] = jnp.zeros_like(work)
    unpack(g_ref, work, u_ref.shape[0] // TILE)
    factor_panels(work, u_ref, lines, high, low)


def reduce_factor_kernel(
    groups, g_ref, u_ref, over_ref, whole, in1, in2, in3, sum1, sum2, send, arrive, work, lines, high, low
):
    pair, plane, line = groups
    width = lax.axis_size("grp")
    me = lax.axis_index("rows") * width + lax.axis_index("grp")
    c, q, b = me % pair, (me // pair) % plane, me // (pair * plane)

    def at(cc, qq, bb):
        index = (bb * plane + qq) * pair + cc
        return (index // width, index % width)

    peers = [at((c + t) % pair, q, b) for t in range(1, pair)]
    peers += [at(c, (q + t) % plane, b) for t in range(1, plane)]
    peers += [at(c, q, (b + t) % line) for t in range(1, line)]
    barrier = pltpu.get_barrier_semaphore()
    for peer in peers:
        pl.semaphore_signal(barrier, inc=1, device_id=peer, device_id_type=MESH)
    pl.semaphore_wait(barrier, len(peers))

    runs = segments(u_ref.shape[0] // TILE)
    copies = {}

    def start(s, stage, t, source, target, peer):
        slot = stage * 4 + t
        copy = pltpu.make_async_remote_copy(
            src_ref=source,
            dst_ref=target,
            send_sem=send.at[s, slot],
            recv_sem=arrive.at[s, slot],
            device_id=peer,
            device_id_type=MESH,
        )
        copy.start()
        copies[s, stage, t] = copy

    def rows(first, count):
        return pl.ds(pl.multiple_of(first, 8), count)

    def sizes(s):
        first, tiles = runs[s]
        first, n1 = first * TILE, tiles * TILE
        return first, n1 // pair, n1 // (pair * plane), n1 // (pair * plane * line)

    def scatter1(s):
        first, n1, n2, n3 = sizes(s)
        for t in range(1, pair):
            other = (c + t) % pair
            start(s, 0, t, g_ref.at[rows(first + other * n1, n1)], in1.at[t - 1, rows(first // pair, n1)], at(other, q, b))

    def scatter2(s):
        first, n1, n2, n3 = sizes(s)
        mine = rows(first // pair, n1)
        total = g_ref[rows(first + c * n1, n1), :]
        for t in range(1, pair):
            copies[s, 0, t].wait_recv()
            total = total + in1[t - 1, mine, :]
        sum1[mine, :] = total
        for t in range(1, plane):
            other = (q + t) % plane
            start(s, 1, t, sum1.at[rows(first // pair + other * n2, n2)], in2.at[t - 1, rows(first // (pair * plane), n2)], at(c, other, b))

    def scatter3(s):
        first, n1, n2, n3 = sizes(s)
        mine = rows(first // (pair * plane), n2)
        total = sum1[rows(first // pair + q * n2, n2), :]
        for t in range(1, plane):
            copies[s, 1, t].wait_recv()
            total = total + in2[t - 1, mine, :]
        sum2[mine, :] = total
        for t in range(1, line):
            other = (b + t) % line
            start(s, 2, t, sum2.at[rows(first // (pair * plane) + other * n3, n3)], in3.at[t - 1, rows(first // (pair * plane * line), n3)], at(c, q, other))

    def gather3(s):
        first, n1, n2, n3 = sizes(s)
        mine = rows(first // (pair * plane * line), n3)
        total = sum2[rows(first // (pair * plane) + b * n3, n3), :]
        for t in range(1, line):
            copies[s, 2, t].wait_recv()
            total = total + in3[t - 1, mine, :]
        here = rows(first + c * n1 + q * n2 + b * n3, n3)
        whole[here, :] = total
        for t in range(1, line):
            start(s, 3, t, whole.at[here], whole.at[here], at(c, q, (b + t) % line))

    def gather2(s):
        first, n1, n2, n3 = sizes(s)
        for t in range(1, line):
            copies[s, 3, t].wait_recv()
        here = rows(first + c * n1 + q * n2, n2)
        for t in range(1, plane):
            start(s, 4, t, whole.at[here], whole.at[here], at(c, (q + t) % plane, b))

    def gather1(s):
        first, n1, n2, n3 = sizes(s)
        for t in range(1, plane):
            copies[s, 4, t].wait_recv()
        here = rows(first + c * n1, n1)
        for t in range(1, pair):
            start(s, 5, t, whole.at[here], whole.at[here], at((c + t) % pair, q, b))

    def finish(s):
        for t in range(1, pair):
            copies[s, 5, t].wait_recv()

    stages = [scatter1, scatter2, scatter3, gather3, gather2, gather1, finish]
    for step in range(len(runs) + len(stages) - 1):
        for k in reversed(range(len(stages))):
            if 0 <= step - k < len(runs):
                stages[k](step - k)
    for copy in copies.values():
        copy.wait_send()
    over_ref[...] = whole[whole.shape[0] - 8 :, :]
    unpack(whole, work, u_ref.shape[0] // TILE)
    factor_panels(work, u_ref, lines, high, low)


def reduce_factor(packed, cols):
    devices = lax.axis_size("rows") * lax.axis_size("grp")
    rows = packed.shape[0]
    common = [
        pltpu.VMEM((cols, cols), jnp.float32),
        pltpu.VMEM((2, 10, 8, TILE), jnp.float32),
        pltpu.VMEM((TILE, cols), jnp.bfloat16),
        pltpu.VMEM((TILE, cols), jnp.bfloat16),
    ]
    call = functools.partial(
        pl.pallas_call,
        out_shape=[jax.ShapeDtypeStruct((cols, cols), jnp.float32), jax.ShapeDtypeStruct((8, TILE), jnp.float32)],
        in_specs=[pl.BlockSpec(memory_space=pltpu.VMEM)],
        out_specs=[pl.BlockSpec(memory_space=pltpu.VMEM)] * 2,
    )
    pair, plane = 2, 4
    line = devices // (pair * plane)
    if devices % (pair * plane) or line > 4 or any(tiles * TILE % (8 * devices) for _, tiles in segments(cols // TILE)):
        return call(
            factor_kernel,
            scratch_shapes=common,
            compiler_params=pltpu.CompilerParams(vmem_limit_bytes=VMEM_LIMIT),
        )(lax.psum(packed, ("rows", "grp")))
    runs = len(segments(cols // TILE))
    return call(
        functools.partial(reduce_factor_kernel, (pair, plane, line)),
        scratch_shapes=[
            pltpu.VMEM((rows, TILE), jnp.float32),
            pltpu.VMEM((pair - 1, rows // pair, TILE), jnp.float32),
            pltpu.VMEM((plane - 1, rows // (pair * plane), TILE), jnp.float32),
            pltpu.VMEM((max(line - 1, 1), rows // devices, TILE), jnp.float32),
            pltpu.VMEM((rows // pair, TILE), jnp.float32),
            pltpu.VMEM((rows // (pair * plane), TILE), jnp.float32),
            pltpu.SemaphoreType.DMA((runs, 24)),
            pltpu.SemaphoreType.DMA((runs, 24)),
            *common,
        ],
        compiler_params=pltpu.CompilerParams(vmem_limit_bytes=VMEM_LIMIT, collective_id=1, has_side_effects=True),
    )(packed)


def exchange_kernel(
    sizes, scale, x_ref, s_ref, h_ref, pick_ref, w_ref, over_ref, g_ref,
    x_in, signed_h, x_out, x_got, mixed, y_out, y_got, high, low, load, send_a, got_a, send_b, got_b,
):
    near, far, ahead = sizes
    steps, rows = x_in.shape[0], x_in.shape[1]
    base, piece, share = h_ref.shape[0], rows // near, pick_ref.shape[0] // far
    width = lax.axis_size("grp")
    me = lax.axis_index("rows") * width + lax.axis_index("grp")
    a, b = me % near, me // near

    def at(aa, bb):
        index = bb * near + aa
        return (index // width, index % width)

    def loading(c):
        lanes = pl.ds(pl.multiple_of(c * TILE, TILE), TILE)
        return pltpu.make_async_copy(x_ref.at[:, lanes], x_in.at[c], load.at[c])

    def span(i, count):
        return pl.ds(pl.multiple_of(i * count, count), count)

    def near_copy(c, t):
        there = (a + t) % near
        return pltpu.make_async_remote_copy(
            src_ref=x_out.at[c, span(there, piece)],
            dst_ref=x_got.at[c, span(a, piece)],
            send_sem=send_a.at[c, t],
            recv_sem=got_a.at[c, t],
            device_id=at(there, b),
            device_id_type=MESH,
        )

    def far_copy(c, t):
        there = (b + t) % far
        return pltpu.make_async_remote_copy(
            src_ref=y_out.at[c, span(there, share)],
            dst_ref=y_got.at[c, span(b, share)],
            send_sem=send_b.at[c, t],
            recv_sem=got_b.at[c, t],
            device_id=at(a, there),
            device_id_type=MESH,
        )

    def each(first, last, act):
        def body(t, carry):
            act(t)
            return carry

        lax.fori_loop(first, last, body, 0)

    def transform(c):
        loading(c).wait()
        parts = []
        for i in range(rows // base):
            x_high, x_low = split(x_in[c, i * base : (i + 1) * base, :])
            part = jnp.dot(signed_h[i], x_high, preferred_element_type=jnp.float32)
            parts.append(part + jnp.dot(signed_h[i], x_low, preferred_element_type=jnp.float32))
        for i, part in enumerate(butterfly(parts)):
            x_out[c, i * base : (i + 1) * base, :] = part
        each(1, near, lambda t: near_copy(c, t).start())
        x_got[c, span(a, piece), :] = x_out[c, span(a, piece), :]

    def middle(c):
        each(1, near, lambda t: near_copy(c, t).wait_recv())
        block = min(32, piece)

        def mix(r):
            where = [pl.ds(pl.multiple_of(j * piece + r * block, block), block) for j in range(near)]
            for here, part in zip(where, butterfly([x_got[c, here, :] for here in where])):
                mixed[here, :] = part

        each(0, piece // block, mix)

        def keep(r):
            for u in range(8):
                y_out[c, pl.ds(pl.multiple_of(r * 8, 8) + u, 1), :] = mixed[pl.ds(pick_ref[r * 8 + u], 1), :]

        each(0, pick_ref.shape[0] // 8, keep)
        each(1, far, lambda t: far_copy(c, t).start())
        y_got[c, span(b, share), :] = y_out[c, span(b, share), :]

    def last(c):
        each(1, far, lambda t: far_copy(c, t).wait_recv())
        lanes = pl.ds(pl.multiple_of(c * TILE, TILE), TILE)

        def mix(r):
            where = [pl.ds(pl.multiple_of(j * share + r * 16, 16), 16) for j in range(far)]
            for here, part in zip(where, butterfly([y_got[c, here, :] for here in where])):
                x_high, x_low = split(part * (w_ref[here, :] * scale))
                high[here, lanes] = x_high
                low[here, lanes] = x_low

        each(0, share // 16, mix)

        def gram(i):
            left = pl.ds(pl.multiple_of(i * TILE, TILE), TILE)
            half = i // 2
            first = 2 * steps * half - 2 * half * (half - 1) + (i % 2) * (steps - 2 * half)
            tile = dot3((high[:, left], low[:, left]), (high[:, lanes], low[:, lanes]), ((0,), (0,)))
            g_ref[span(first + c - i, TILE), :] = tile

        each(0, c + 1, gram)

    each(0, steps, lambda c: loading(c).start())
    barrier = pltpu.get_barrier_semaphore()

    def greet(there):
        pl.semaphore_signal(barrier, inc=1, device_id=there, device_id_type=MESH)

    each(1, near, lambda t: greet(at((a + t) % near, b)))
    each(1, far, lambda t: greet(at(a, (b + t) % far)))
    for i in range(rows // base):
        signed_h[i] = (h_ref[...] * s_ref[i : i + 1, :]).astype(jnp.bfloat16)
    sizes_list, starts = panel_tiles(steps)
    for i in range(1, steps, 2):
        spare = (starts[i] + sizes_list[i] - 1) * TILE
        g_ref[spare : spare + TILE, :] = jnp.zeros((TILE, TILE), jnp.float32)
    g_ref[g_ref.shape[0] - 8 :, :] = over_ref[...]
    pl.semaphore_wait(barrier, near + far - 2)
    each(0, ahead, transform)

    def step(c):
        @pl.when(c + ahead < steps)
        def _():
            transform(c + ahead)

        middle(c)

        @pl.when(c > 0)
        def _():
            last(c - 1)

    each(0, steps, step)
    last(steps - 1)
    each(0, steps, lambda c: each(1, near, lambda t: near_copy(c, t).wait_send()))
    each(0, steps, lambda c: each(1, far, lambda t: far_copy(c, t).wait_send()))


def exchange(matrix, row_signs, all_indices, near, far, room, scale):
    rows, cols = matrix.shape
    steps, piece, share = cols // TILE, rows // near, room // far
    base = min(256, rows)
    width = lax.axis_size("grp")
    me = lax.axis_index("rows") * width + lax.axis_index("grp")
    a, b = me % near, me // near
    blocks = near * far
    within = all_indices - (jnp.arange(blocks, dtype=jnp.int32)[:, None] * rows + a * piece)
    hits = within[:, None, :] == jnp.arange(piece, dtype=jnp.int32)[None, :, None]
    taken = jnp.max(hits.astype(jnp.float32), axis=2).reshape(far, rows)
    needed = jnp.max(taken, axis=0).reshape(rows // TILE, TILE)
    lane = jnp.arange(TILE)
    before = jnp.dot(needed, (lane[:, None] < lane[None, :]).astype(jnp.float32), preferred_element_type=jnp.float32)
    line_sum = jnp.sum(needed, axis=1)
    line = jnp.arange(rows // TILE)
    before = before + jnp.sum(jnp.where(line[None, :] < line[:, None], line_sum[None, :], 0.0), axis=1)[:, None]
    slot = jnp.where(needed > 0, before, -1.0).reshape(rows).astype(jnp.int32)
    hot = jnp.arange(room, dtype=jnp.int32)[:, None] == slot[None, :]
    row = jnp.arange(rows, dtype=jnp.int32)
    pick = jnp.sum(jnp.where(hot, row[None, :], 0), axis=1)
    mine = lax.dynamic_slice_in_dim(hot, b * share, share, 0)
    weights = jnp.max(jnp.where(mine[None, :, :], taken[:, None, :], 0.0), axis=2)
    weights = jnp.broadcast_to(weights.reshape(room, 1), (room, TILE))
    over = (jnp.sum(line_sum) > room).astype(jnp.float32)
    over = jnp.broadcast_to(over, (8, TILE))
    tiles = sum(panel_tiles(steps)[0])
    vmem = pl.BlockSpec(memory_space=pltpu.VMEM)
    return pl.pallas_call(
        functools.partial(exchange_kernel, (near, far, min(3, steps)), scale),
        out_shape=jax.ShapeDtypeStruct((tiles * TILE, TILE), jnp.float32),
        in_specs=[pl.BlockSpec(memory_space=pl.ANY), vmem, vmem, pl.BlockSpec(memory_space=pltpu.SMEM), vmem, vmem],
        out_specs=vmem,
        scratch_shapes=[
            pltpu.VMEM((steps, rows, TILE), jnp.float32),
            pltpu.VMEM((rows // base, base, base), jnp.bfloat16),
            pltpu.VMEM((steps, rows, TILE), jnp.float32),
            pltpu.VMEM((steps, rows, TILE), jnp.float32),
            pltpu.VMEM((rows, TILE), jnp.float32),
            pltpu.VMEM((steps, room, TILE), jnp.float32),
            pltpu.VMEM((steps, room, TILE), jnp.float32),
            pltpu.VMEM((room, cols), jnp.bfloat16),
            pltpu.VMEM((room, cols), jnp.bfloat16),
            pltpu.SemaphoreType.DMA((steps,)),
            pltpu.SemaphoreType.DMA((steps, near)),
            pltpu.SemaphoreType.DMA((steps, near)),
            pltpu.SemaphoreType.DMA((steps, far)),
            pltpu.SemaphoreType.DMA((steps, far)),
        ],
        compiler_params=pltpu.CompilerParams(vmem_limit_bytes=VMEM_LIMIT, collective_id=2, has_side_effects=True),
    )(matrix, row_signs.astype(jnp.float32).reshape(rows // base, base), sylvester(base), pick, weights, over)


def whole_exchange(matrix, row_signs, all_indices, scale):
    blocks = lax.axis_size("rows") * lax.axis_size("grp")
    row_dev, col_count = matrix.shape
    piece_rows = row_dev // blocks
    position = lax.axis_index(("rows", "grp"))
    signs = jnp.broadcast_to(row_signs.astype(jnp.float32)[:, None], (row_dev, TILE))
    before = local_transform(matrix, signs, min(256, row_dev))
    arrived = lax.all_to_all(
        before.reshape(blocks, piece_rows, col_count),
        ("rows", "grp"),
        split_axis=0,
        concat_axis=0,
        tiled=True,
    )
    first = jnp.arange(blocks, dtype=jnp.int32)[:, None] * row_dev + position * piece_rows
    within = all_indices - first
    hits = within[:, None, :] == jnp.arange(piece_rows, dtype=jnp.int32)[None, :, None]
    weights = jnp.max(hits.astype(jnp.float32), axis=2)
    weights = jnp.broadcast_to(weights[:, :, None], (blocks, piece_rows, TILE))
    half = gram_share(arrived, weights, scale)
    whole = (half + half.T) * 0.5
    pieces = []
    for i, count in enumerate(panel_tiles(col_count // TILE)[0]):
        row = whole[i * TILE : (i + 1) * TILE]
        tiles = [row[:, j * TILE : (j + 1) * TILE] for j in range(i, col_count // TILE)]
        tiles += [jnp.zeros((TILE, TILE), jnp.float32)] * (count - len(tiles))
        pieces += tiles
    return jnp.concatenate(pieces, axis=0)


def shards(matrix, row_signs, samples):
    count_rows = lax.axis_size("rows")
    blocks = count_rows * lax.axis_size("grp")
    row_dev, col_count = matrix.shape
    sample_dev = samples.shape[0]
    scale = (sample_dev * blocks) ** -0.5
    all_indices = lax.all_gather(samples, ("rows", "grp"), axis=0)
    far = 4
    near = blocks // far
    chance = 1.0 - (1.0 - sample_dev / row_dev) ** far
    room = row_dev * chance + 5.0 * (row_dev * chance * (1.0 - chance)) ** 0.5
    room = min(row_dev, -(-int(room) // (16 * far)) * 16 * far)
    share_rows = col_count // count_rows

    def own(upper_factor):
        return lax.dynamic_slice_in_dim(upper_factor, lax.axis_index("rows") * share_rows, share_rows, 0)

    packed = exchange(matrix, row_signs, all_indices, near, far, room, scale)
    upper_factor, over = reduce_factor(packed, col_count)

    def again():
        packed = whole_exchange(matrix, row_signs, all_indices, scale)
        return own(reduce_factor(packed, col_count)[0])

    return lax.cond(over[0, 0] > 0.0, again, lambda: own(upper_factor))


def solution(mesh):
    return jax.shard_map(
        shards,
        mesh=mesh,
        in_specs=(P(("rows", "grp"), None), P(("rows", "grp")), P(("rows", "grp"))),
        out_specs=P("rows", None),
        check_vma=False,
    )
```

```python
import functools

import jax
import jax.numpy as jnp
from jax import lax
from jax.experimental import pallas as pl
from jax.experimental.pallas import tpu as pltpu
from jax.sharding import PartitionSpec as P

MESH = pl.DeviceIdType.MESH
VMEM_LIMIT = 60 * 1024 * 1024
TILE = 128


def sylvester(length):
    matrix = jnp.ones((1, 1), jnp.float32)
    while matrix.shape[0] < length:
        matrix = jnp.block([[matrix, matrix], [matrix, -matrix]])
    return matrix


def butterfly(parts):
    span = 1
    while span < len(parts):
        parts = list(parts)
        for start in range(0, len(parts), 2 * span):
            for i in range(start, start + span):
                low, high = parts[i], parts[i + span]
                parts[i], parts[i + span] = low + high, low - high
        span *= 2
    return parts


def split(x):
    high = x.astype(jnp.bfloat16)
    return high, (x - high.astype(jnp.float32)).astype(jnp.bfloat16)


def local_kernel(base, x_ref, s_ref, h_ref, o_ref):
    parts = []
    for i in range(x_ref.shape[0] // base):
        rows = slice(i * base, (i + 1) * base)
        high, low = split(x_ref[rows, :] * s_ref[rows, :])
        both = jnp.dot(h_ref[...], high, preferred_element_type=jnp.float32)
        both += jnp.dot(h_ref[...], low, preferred_element_type=jnp.float32)
        parts.append(both)
    for i, part in enumerate(butterfly(parts)):
        o_ref[i * base : (i + 1) * base, :] = part


def local_transform(matrix, signs, base):
    rows, cols = matrix.shape
    return pl.pallas_call(
        functools.partial(local_kernel, base),
        grid=(cols // TILE,),
        out_shape=jax.ShapeDtypeStruct((rows, cols), jnp.float32),
        in_specs=[
            pl.BlockSpec((rows, TILE), lambda c: (0, c)),
            pl.BlockSpec((rows, TILE), lambda c: (0, 0)),
            pl.BlockSpec((base, base), lambda c: (0, 0)),
        ],
        out_specs=pl.BlockSpec((rows, TILE), lambda c: (0, c)),
        compiler_params=pltpu.CompilerParams(vmem_limit_bytes=VMEM_LIMIT),
    )(matrix, signs, sylvester(base).astype(jnp.bfloat16))


def gram_kernel(scale, x_ref, w_ref, o_ref, left, right):
    blocks, step, cols = x_ref.shape
    rows = blocks * step

    @pl.when(pl.program_id(0) == 0)
    def _():
        o_ref[...] = jnp.zeros_like(o_ref)

    def mix(c, carry):
        at = pl.ds(pl.multiple_of(c * TILE, TILE), TILE)
        parts = butterfly([x_ref[b, :, at] for b in range(blocks)])
        for b in range(0, blocks, 2):
            x = jnp.concatenate(parts[b : b + 2], axis=0) * scale
            w = jnp.concatenate([w_ref[b], w_ref[b + 1]], axis=0)
            high, low = split(x)
            here = slice(b * step, (b + 2) * step)
            there = slice(rows + b * step, rows + (b + 2) * step)
            masked = (high.astype(jnp.float32) * w).astype(jnp.bfloat16)
            left[here, at] = masked
            right[here, at] = high
            left[there, at] = masked
            right[there, at] = (2.0 * low.astype(jnp.float32)).astype(jnp.bfloat16)
        return carry

    lax.fori_loop(0, cols // TILE, mix, 0)
    wide = 2 * TILE

    def add(n, carry):
        at = pl.ds(pl.multiple_of(n * wide, wide), wide)
        o_ref[:, at] += lax.dot_general(
            left[...], right[:, at], (((0,), (0,)), ((), ())), preferred_element_type=jnp.float32
        )
        return carry

    lax.fori_loop(0, cols // wide, add, 0)


def gram_share(arrived, weights, scale):
    blocks, piece, cols = arrived.shape
    step = 8
    return pl.pallas_call(
        functools.partial(gram_kernel, scale),
        grid=(piece // step,),
        out_shape=jax.ShapeDtypeStruct((cols, cols), jnp.float32),
        in_specs=[
            pl.BlockSpec((blocks, step, cols), lambda t: (0, t, 0)),
            pl.BlockSpec((blocks, step, TILE), lambda t: (0, t, 0)),
        ],
        out_specs=pl.BlockSpec((cols, cols), lambda t: (0, 0)),
        scratch_shapes=[pltpu.VMEM((2 * blocks * step, cols), jnp.bfloat16)] * 2,
        compiler_params=pltpu.CompilerParams(vmem_limit_bytes=VMEM_LIMIT),
    )(arrived, weights)


def panel_tiles(panels):
    sizes = [panels - i + (panels - i) % 2 for i in range(panels)]
    return sizes, [sum(sizes[:i]) for i in range(panels)]


def segments(panels):
    sizes, starts = panel_tiles(panels)
    runs = [(0, 1), (1, 2), (2, 4), (4, panels)]
    return [(starts[i], sum(sizes[i:j])) for i, j in runs]


def dot3(a, b, dims):
    (ah, al), (bh, bl) = a, b
    go = functools.partial(lax.dot_general, dimension_numbers=(dims, ((), ())), preferred_element_type=jnp.float32)
    return go(ah, bh) + (go(ah, bl) + go(al, bh))

def spread(row):
    return jnp.broadcast_to(row, (8, TILE))

def factor_block(block, lines):
    count, group = TILE // 8, 4
    sub_id = lax.broadcasted_iota(jnp.int32, (8, TILE), 0)
    lane_id = lax.broadcasted_iota(jnp.int32, (8, TILE), 1)
    strips = [block[8 * i : 8 * i + 8, :] for i in range(count)]
    inverse = [(lane_id == sub_id + 8 * i).astype(jnp.float32) for i in range(count)]
    for first in range(0, count, group):
        last = first + group
        for s in range(first, last):
            columns = {
                i: [jnp.broadcast_to(strips[i][:, 8 * s + t : 8 * s + t + 1], (8, TILE)) for t in range(8)]
                for i in range(s, last)
            }
            for t in range(8):
                lines[s % 2, t] = columns[s][t]
            lines[s % 2, 8] = strips[s]
            lines[s % 2, 9] = inverse[s]
            pivot = {(r, t): spread(lines[s % 2, t, r : r + 1, :]) for t in range(8) for r in range(t, 8)}
            row = [spread(lines[s % 2, 8, q : q + 1, :]) for q in range(8)]
            inv_row = [spread(lines[s % 2, 9, q : q + 1, :]) for q in range(8)]
            for j in range(8):
                root = lax.rsqrt(pivot[j, j])
                for r in range(j + 1, 8):
                    pivot[r, j] = pivot[r, j] * root
                for t in range(j + 1, 8):
                    for r in range(t, 8):
                        pivot[r, t] = pivot[r, t] - pivot[r, j] * pivot[t, j]
                row[j] = row[j] * root
                inv_row[j] = inv_row[j] * root
                for r in range(j + 1, 8):
                    row[r] = row[r] - pivot[r, j] * row[j]
                    inv_row[r] = inv_row[r] - pivot[r, j] * inv_row[j]
                for i in range(s + 1, last):
                    left = columns[i]
                    left[j] = left[j] * root
                    for r in range(j + 1, 8):
                        left[r] = left[r] - pivot[r, j] * left[j]
                    strips[i] = strips[i] - left[j] * row[j]
                    inverse[i] = inverse[i] - left[j] * inv_row[j]
            for q in range(8):
                strips[s] = row[q] if q == 0 else jnp.where(sub_id == q, row[q], strips[s])
                inverse[s] = inv_row[q] if q == 0 else jnp.where(sub_id == q, inv_row[q], inverse[s])
        if last < count:
            high, low = split(jnp.concatenate(strips[first:last], axis=0))
            inv_high, inv_low = split(jnp.concatenate(inverse[first:last], axis=0))
            three = jnp.concatenate([high, low, high], axis=0)
            rest = jnp.concatenate([high, high, low], axis=0)
            inv_rest = jnp.concatenate([inv_high, inv_high, inv_low], axis=0)
            both = jnp.concatenate([rest, inv_rest], axis=1)
            change = lax.dot_general(three, both, (((0,), (0,)), ((), ())), preferred_element_type=jnp.float32)
            for i in range(last, count):
                strips[i] = strips[i] - change[8 * i : 8 * i + 8, :TILE]
                inverse[i] = inverse[i] - change[8 * i : 8 * i + 8, TILE:]
    return jnp.concatenate(inverse, axis=0)


def factor_panels(work, u_ref, lines, high, low):
    cols = u_ref.shape[0]

    def panel(k, carry):
        base = pl.multiple_of(k * TILE, TILE)
        here = pl.ds(base, TILE)
        lower = split(factor_block(work[here, here], lines))
        wide_row = lax.broadcasted_iota(jnp.int32, (TILE, cols), 0) + base
        wide_lane = lax.broadcasted_iota(jnp.int32, (TILE, cols), 1)
        upper = dot3(lower, split(work[here, :]), ((1,), (0,)))
        upper = jnp.where(wide_lane >= wide_row, upper, 0.0)
        u_ref[here, :] = upper
        high[...], low[...] = split(upper)

        def trail(start, i, inner):
            there = pl.ds(pl.multiple_of(i * TILE, TILE), TILE)
            right = (high[:, start:], low[:, start:])
            work[there, start:] -= dot3((high[:, there], low[:, there]), right, ((0,), (0,)))
            return inner

        half = cols // TILE // 2
        lax.fori_loop(k + 1, half, functools.partial(trail, 0), 0)
        lax.fori_loop(jnp.maximum(k + 1, half), cols // TILE, functools.partial(trail, cols // 2), 0)
        return carry

    lax.fori_loop(0, cols // TILE, panel, 0)


def unpack(source, work, panels):
    for i, start in enumerate(panel_tiles(panels)[1]):
        for j in range(i, panels):
            p = (start + j - i) * TILE
            work[i * TILE : (i + 1) * TILE, j * TILE : (j + 1) * TILE] = source[p : p + TILE, :]


def factor_kernel(g_ref, u_ref, over_ref, work, lines, high, low):
    over_ref[...] = g_ref[g_ref.shape[0] - 8 :, :]
    work[...] = jnp.zeros_like(work)
    unpack(g_ref, work, u_ref.shape[0] // TILE)
    factor_panels(work, u_ref, lines, high, low)


def reduce_factor_kernel(
    groups, g_ref, u_ref, over_ref, whole, in1, in2, in3, sum1, sum2, send, arrive, work, lines, high, low
):
    pair, plane, line = groups
    width = lax.axis_size("grp")
    me = lax.axis_index("rows") * width + lax.axis_index("grp")
    c, q, b = me % pair, (me // pair) % plane, me // (pair * plane)

    def at(cc, qq, bb):
        index = (bb * plane + qq) * pair + cc
        return (index // width, index % width)

    peers = [at((c + t) % pair, q, b) for t in range(1, pair)]
    peers += [at(c, (q + t) % plane, b) for t in range(1, plane)]
    peers += [at(c, q, (b + t) % line) for t in range(1, line)]
    barrier = pltpu.get_barrier_semaphore()
    for peer in peers:
        pl.semaphore_signal(barrier, inc=1, device_id=peer, device_id_type=MESH)
    pl.semaphore_wait(barrier, len(peers))

    runs = segments(u_ref.shape[0] // TILE)
    copies = {}

    def start(s, stage, t, source, target, peer):
        slot = stage * 4 + t
        copy = pltpu.make_async_remote_copy(
            src_ref=source,
            dst_ref=target,
            send_sem=send.at[s, slot],
            recv_sem=arrive.at[s, slot],
            device_id=peer,
            device_id_type=MESH,
        )
        copy.start()
        copies[s, stage, t] = copy

    def rows(first, count):
        return pl.ds(pl.multiple_of(first, 8), count)

    def sizes(s):
        first, tiles = runs[s]
        first, n1 = first * TILE, tiles * TILE
        return first, n1 // pair, n1 // (pair * plane), n1 // (pair * plane * line)

    def scatter1(s):
        first, n1, n2, n3 = sizes(s)
        for t in range(1, pair):
            other = (c + t) % pair
            start(s, 0, t, g_ref.at[rows(first + other * n1, n1)], in1.at[t - 1, rows(first // pair, n1)], at(other, q, b))

    def scatter2(s):
        first, n1, n2, n3 = sizes(s)
        mine = rows(first // pair, n1)
        total = g_ref[rows(first + c * n1, n1), :]
        for t in range(1, pair):
            copies[s, 0, t].wait_recv()
            total = total + in1[t - 1, mine, :]
        sum1[mine, :] = total
        for t in range(1, plane):
            other = (q + t) % plane
            start(s, 1, t, sum1.at[rows(first // pair + other * n2, n2)], in2.at[t - 1, rows(first // (pair * plane), n2)], at(c, other, b))

    def scatter3(s):
        first, n1, n2, n3 = sizes(s)
        mine = rows(first // (pair * plane), n2)
        total = sum1[rows(first // pair + q * n2, n2), :]
        for t in range(1, plane):
            copies[s, 1, t].wait_recv()
            total = total + in2[t - 1, mine, :]
        sum2[mine, :] = total
        for t in range(1, line):
            other = (b + t) % line
            start(s, 2, t, sum2.at[rows(first // (pair * plane) + other * n3, n3)], in3.at[t - 1, rows(first // (pair * plane * line), n3)], at(c, q, other))

    def gather3(s):
        first, n1, n2, n3 = sizes(s)
        mine = rows(first // (pair * plane * line), n3)
        total = sum2[rows(first // (pair * plane) + b * n3, n3), :]
        for t in range(1, line):
            copies[s, 2, t].wait_recv()
            total = total + in3[t - 1, mine, :]
        here = rows(first + c * n1 + q * n2 + b * n3, n3)
        whole[here, :] = total
        for t in range(1, line):
            start(s, 3, t, whole.at[here], whole.at[here], at(c, q, (b + t) % line))

    def gather2(s):
        first, n1, n2, n3 = sizes(s)
        for t in range(1, line):
            copies[s, 3, t].wait_recv()
        here = rows(first + c * n1 + q * n2, n2)
        for t in range(1, plane):
            start(s, 4, t, whole.at[here], whole.at[here], at(c, (q + t) % plane, b))

    def gather1(s):
        first, n1, n2, n3 = sizes(s)
        for t in range(1, plane):
            copies[s, 4, t].wait_recv()
        here = rows(first + c * n1, n1)
        for t in range(1, pair):
            start(s, 5, t, whole.at[here], whole.at[here], at((c + t) % pair, q, b))

    def finish(s):
        for t in range(1, pair):
            copies[s, 5, t].wait_recv()

    stages = [scatter1, scatter2, scatter3, gather3, gather2, gather1, finish]
    for step in range(len(runs) + len(stages) - 1):
        for k in reversed(range(len(stages))):
            if 0 <= step - k < len(runs):
                stages[k](step - k)
    for copy in copies.values():
        copy.wait_send()
    over_ref[...] = whole[whole.shape[0] - 8 :, :]
    unpack(whole, work, u_ref.shape[0] // TILE)
    factor_panels(work, u_ref, lines, high, low)


def reduce_factor(packed, cols):
    devices = lax.axis_size("rows") * lax.axis_size("grp")
    rows = packed.shape[0]
    common = [
        pltpu.VMEM((cols, cols), jnp.float32),
        pltpu.VMEM((2, 10, 8, TILE), jnp.float32),
        pltpu.VMEM((TILE, cols), jnp.bfloat16),
        pltpu.VMEM((TILE, cols), jnp.bfloat16),
    ]
    call = functools.partial(
        pl.pallas_call,
        out_shape=[jax.ShapeDtypeStruct((cols, cols), jnp.float32), jax.ShapeDtypeStruct((8, TILE), jnp.float32)],
        in_specs=[pl.BlockSpec(memory_space=pltpu.VMEM)],
        out_specs=[pl.BlockSpec(memory_space=pltpu.VMEM)] * 2,
    )
    pair, plane = 2, 4
    line = devices // (pair * plane)
    if devices % (pair * plane) or line > 4 or any(tiles * TILE % (8 * devices) for _, tiles in segments(cols // TILE)):
        return call(
            factor_kernel,
            scratch_shapes=common,
            compiler_params=pltpu.CompilerParams(vmem_limit_bytes=VMEM_LIMIT),
        )(lax.psum(packed, ("rows", "grp")))
    runs = len(segments(cols // TILE))
    return call(
        functools.partial(reduce_factor_kernel, (pair, plane, line)),
        scratch_shapes=[
            pltpu.VMEM((rows, TILE), jnp.float32),
            pltpu.VMEM((pair - 1, rows // pair, TILE), jnp.float32),
            pltpu.VMEM((plane - 1, rows // (pair * plane), TILE), jnp.float32),
            pltpu.VMEM((max(line - 1, 1), rows // devices, TILE), jnp.float32),
            pltpu.VMEM((rows // pair, TILE), jnp.float32),
            pltpu.VMEM((rows // (pair * plane), TILE), jnp.float32),
            pltpu.SemaphoreType.DMA((runs, 24)),
            pltpu.SemaphoreType.DMA((runs, 24)),
            *common,
        ],
        compiler_params=pltpu.CompilerParams(vmem_limit_bytes=VMEM_LIMIT, collective_id=1, has_side_effects=True),
    )(packed)


def exchange_kernel(
    sizes, scale, x_ref, s_ref, h_ref, samples_ref, g_ref,
    x_in, signed_h, x_out, x_got, mixed, y_out, y_got, high, low, samples, taken, weights, pick_row, pick_ref,
    load, send_a, got_a, send_b, got_b, send_s, got_s,
):
    near, far, ahead = sizes
    steps, rows = x_in.shape[0], x_in.shape[1]
    base, piece, share = h_ref.shape[0], rows // near, weights.shape[0] // far
    room = share * far
    width = lax.axis_size("grp")
    me = lax.axis_index("rows") * width + lax.axis_index("grp")
    a, b = me % near, me // near

    def at(aa, bb):
        index = bb * near + aa
        return (index // width, index % width)

    def loading(c):
        lanes = pl.ds(pl.multiple_of(c * TILE, TILE), TILE)
        return pltpu.make_async_copy(x_ref.at[:, lanes], x_in.at[c], load.at[c])

    def span(i, count):
        return pl.ds(pl.multiple_of(i * count, count), count)

    def near_copy(c, t):
        there = (a + t) % near
        return pltpu.make_async_remote_copy(
            src_ref=x_out.at[c, span(there, piece)],
            dst_ref=x_got.at[c, span(a, piece)],
            send_sem=send_a.at[c, t],
            recv_sem=got_a.at[c, t],
            device_id=at(there, b),
            device_id_type=MESH,
        )

    def far_copy(c, t):
        there = (b + t) % far
        return pltpu.make_async_remote_copy(
            src_ref=y_out.at[c, span(there, share)],
            dst_ref=y_got.at[c, span(b, share)],
            send_sem=send_b.at[c, t],
            recv_sem=got_b.at[c, t],
            device_id=at(a, there),
            device_id_type=MESH,
        )

    def each(first, last, act):
        def body(t, carry):
            act(t)
            return carry

        lax.fori_loop(first, last, body, 0)

    def picked(group, offset):
        return jnp.minimum(jnp.maximum(pick_ref[group, offset], 0), rows - 1)

    def sample_copy(t, along):
        there = at((a + t) % near, b) if along == 0 else at(a, (b + t) % far)
        source = samples_ref if along == 0 else samples.at[pl.ds(b * near, near)]
        target = samples.at[me] if along == 0 else samples.at[pl.ds(b * near, near)]
        return pltpu.make_async_remote_copy(
            src_ref=source,
            dst_ref=target,
            send_sem=send_s.at[along * near + t],
            recv_sem=got_s.at[along * near + t],
            device_id=there,
            device_id_type=MESH,
        )

    def choose():
        lines = samples_ref.shape[0]
        position = lax.broadcasted_iota(jnp.int32, (piece, TILE), 0)
        ones = jnp.ones((TILE, TILE), jnp.bfloat16)

        def presence(kl):
            where = pl.ds(pl.multiple_of(kl * piece, piece), piece)
            for kz in range(far):
                block = kz * near + kl
                hits = jnp.zeros((piece, TILE), jnp.float32)
                for i in range(lines):
                    within = samples[block, i : i + 1, :] - (block * rows + a * piece)
                    hits += jnp.where(position == within, 1.0, 0.0)
                taken[kz, where, :] = jnp.dot(hits.astype(jnp.bfloat16), ones, preferred_element_type=jnp.float32)

        each(0, near, presence)
        row_id = lax.broadcasted_iota(jnp.int32, (TILE, TILE), 0)
        lane_id = lax.broadcasted_iota(jnp.int32, (TILE, TILE), 1)
        earlier = jnp.where(lane_id < row_id, 1.0, 0.0).astype(jnp.bfloat16)
        total = jnp.zeros((1, TILE), jnp.float32)
        for i in range(rows // TILE):
            here = slice(i * TILE, (i + 1) * TILE)
            need = taken[0, here, :]
            for kz in range(1, far):
                need = jnp.maximum(need, taken[kz, here, :])
            rank = jnp.dot(earlier, need.astype(jnp.bfloat16), preferred_element_type=jnp.float32)
            mixed[here, :] = jnp.where(need > 0.0, rank + total, -1.0)
            total = total + rank[TILE - 1 :, :] + need[TILE - 1 :, :]
        lane = lax.broadcasted_iota(jnp.int32, (8, TILE), 1).astype(jnp.float32)
        sub = lax.broadcasted_iota(jnp.int32, (8, TILE), 0).astype(jnp.float32)
        tiles = pick_row.shape[0]

        def find(r, found):
            for u in range(4):
                slot = mixed[pl.ds(pl.multiple_of(r * 32 + u * 8, 8), 8), :]
                number = sub + (r * 32 + u * 8).astype(jnp.float32)
                found = tuple(f + jnp.where(slot == lane + float(v * TILE), number, 0.0) for v, f in enumerate(found))
            return found

        found = lax.fori_loop(0, rows // 32, find, (jnp.zeros((8, TILE), jnp.float32),) * tiles)
        for v in range(tiles):
            pick_row[v : v + 1, :] = jnp.sum(found[v], axis=0, keepdims=True).astype(jnp.int32)
        copy = pltpu.make_async_copy(pick_row, pick_ref, load.at[steps])
        copy.start()
        copy.wait()

        def weigh(r):
            for u in range(8):
                place = b * share + r * 8 + u
                row = picked(place // TILE, place % TILE)
                for kz in range(far):
                    weights[pl.ds(pl.multiple_of(kz * share + r * 8, 8) + u, 1), :] = taken[kz, pl.ds(row, 1), :]

        each(0, share // 8, weigh)
        slot = lax.broadcasted_iota(jnp.int32, (share, TILE), 0) + b * share
        used = jnp.where(slot.astype(jnp.float32) < total, scale, 0.0)
        for kz in range(far):
            here = slice(kz * share, (kz + 1) * share)
            weights[here, :] = weights[here, :] * used
        g_ref[g_ref.shape[0] - 8 :, :] = jnp.broadcast_to(jnp.where(total > float(room), 1.0, 0.0), (8, TILE))

    def transform(c):
        loading(c).wait()
        parts = []
        for i in range(rows // base):
            x_high, x_low = split(x_in[c, i * base : (i + 1) * base, :])
            part = jnp.dot(signed_h[i], x_high, preferred_element_type=jnp.float32)
            parts.append(part + jnp.dot(signed_h[i], x_low, preferred_element_type=jnp.float32))
        for i, part in enumerate(butterfly(parts)):
            x_out[c, i * base : (i + 1) * base, :] = part
        each(1, near, lambda t: near_copy(c, t).start())
        x_got[c, span(a, piece), :] = x_out[c, span(a, piece), :]

    def middle(c):
        each(1, near, lambda t: near_copy(c, t).wait_recv())
        block = min(32, piece)

        def mix(r):
            where = [pl.ds(pl.multiple_of(j * piece + r * block, block), block) for j in range(near)]
            for here, part in zip(where, butterfly([x_got[c, here, :] for here in where])):
                mixed[here, :] = part

        each(0, piece // block, mix)

        def keep(r):
            group, offset = (r * 32) // TILE, (r * 32) % TILE
            kept = [mixed[pl.ds(picked(group, offset + u), 1), :] for u in range(32)]
            for u in range(0, 32, 8):
                y_out[c, pl.ds(pl.multiple_of(r * 32 + u, 8), 8), :] = jnp.concatenate(kept[u : u + 8], axis=0)

        each(0, room // 32, keep)
        each(1, far, lambda t: far_copy(c, t).start())
        y_got[c, span(b, share), :] = y_out[c, span(b, share), :]

    def last(c):
        each(1, far, lambda t: far_copy(c, t).wait_recv())
        lanes = pl.ds(pl.multiple_of(c * TILE, TILE), TILE)

        def mix(r):
            where = [pl.ds(pl.multiple_of(j * share + r * 16, 16), 16) for j in range(far)]
            for here, part in zip(where, butterfly([y_got[c, here, :] for here in where])):
                x_high, x_low = split(part * weights[here, :])
                high[here, lanes] = x_high
                low[here, lanes] = x_low

        each(0, share // 16, mix)

        def gram(i):
            left = pl.ds(pl.multiple_of(i * TILE, TILE), TILE)
            half = i // 2
            first = 2 * steps * half - 2 * half * (half - 1) + (i % 2) * (steps - 2 * half)
            tile = dot3((high[:, left], low[:, left]), (high[:, lanes], low[:, lanes]), ((0,), (0,)))
            g_ref[span(first + c - i, TILE), :] = tile

        each(0, c + 1, gram)

    each(0, steps, lambda c: loading(c).start())
    barrier = pltpu.get_barrier_semaphore()

    def greet(there):
        pl.semaphore_signal(barrier, inc=1, device_id=there, device_id_type=MESH)

    each(1, near, lambda t: greet(at((a + t) % near, b)))
    each(1, far, lambda t: greet(at(a, (b + t) % far)))
    for i in range(rows // base):
        signed_h[i] = (h_ref[...] * s_ref[i : i + 1, :]).astype(jnp.bfloat16)
    sizes_list, starts = panel_tiles(steps)
    for i in range(1, steps, 2):
        spare = (starts[i] + sizes_list[i] - 1) * TILE
        g_ref[spare : spare + TILE, :] = jnp.zeros((TILE, TILE), jnp.float32)
    samples[me] = samples_ref[...]
    pl.semaphore_wait(barrier, near + far - 2)
    each(1, near, lambda t: sample_copy(t, 0).start())
    transform(0)
    each(1, near, lambda t: sample_copy(t, 0).wait_recv())
    each(1, far, lambda t: sample_copy(t, 1).start())
    each(1, ahead, transform)
    each(1, far, lambda t: sample_copy(t, 1).wait_recv())
    choose()

    def step(c):
        @pl.when(c + ahead < steps)
        def _():
            transform(c + ahead)

        middle(c)

        @pl.when(c > 0)
        def _():
            last(c - 1)

    each(0, steps, step)
    last(steps - 1)
    each(1, near, lambda t: sample_copy(t, 0).wait_send())
    each(1, far, lambda t: sample_copy(t, 1).wait_send())
    each(0, steps, lambda c: each(1, near, lambda t: near_copy(c, t).wait_send()))
    each(0, steps, lambda c: each(1, far, lambda t: far_copy(c, t).wait_send()))


def exchange(matrix, row_signs, samples, near, far, room, scale):
    rows, cols = matrix.shape
    steps = cols // TILE
    base = min(256, rows)
    lines = -(-samples.shape[0] // TILE)
    padded = jnp.pad(samples, (0, lines * TILE - samples.shape[0]), constant_values=-1).reshape(lines, TILE)
    tiles = sum(panel_tiles(steps)[0])
    vmem = pl.BlockSpec(memory_space=pltpu.VMEM)
    picks = -(-room // TILE)
    return pl.pallas_call(
        functools.partial(exchange_kernel, (near, far, min(3, steps)), scale),
        out_shape=jax.ShapeDtypeStruct((tiles * TILE, TILE), jnp.float32),
        in_specs=[pl.BlockSpec(memory_space=pl.ANY), vmem, vmem, vmem],
        out_specs=vmem,
        scratch_shapes=[
            pltpu.VMEM((steps, rows, TILE), jnp.float32),
            pltpu.VMEM((rows // base, base, base), jnp.bfloat16),
            pltpu.VMEM((steps, rows, TILE), jnp.float32),
            pltpu.VMEM((steps, rows, TILE), jnp.float32),
            pltpu.VMEM((rows, TILE), jnp.float32),
            pltpu.VMEM((steps, room, TILE), jnp.float32),
            pltpu.VMEM((steps, room, TILE), jnp.float32),
            pltpu.VMEM((room, cols), jnp.bfloat16),
            pltpu.VMEM((room, cols), jnp.bfloat16),
            pltpu.VMEM((near * far, lines, TILE), jnp.int32),
            pltpu.VMEM((far, rows, TILE), jnp.float32),
            pltpu.VMEM((room, TILE), jnp.float32),
            pltpu.VMEM((picks, TILE), jnp.int32),
            pltpu.SMEM((picks, TILE), jnp.int32),
            pltpu.SemaphoreType.DMA((steps + 1,)),
            pltpu.SemaphoreType.DMA((steps, near)),
            pltpu.SemaphoreType.DMA((steps, near)),
            pltpu.SemaphoreType.DMA((steps, far)),
            pltpu.SemaphoreType.DMA((steps, far)),
            pltpu.SemaphoreType.DMA((near + far,)),
            pltpu.SemaphoreType.DMA((near + far,)),
        ],
        compiler_params=pltpu.CompilerParams(vmem_limit_bytes=VMEM_LIMIT, collective_id=2, has_side_effects=True),
    )(matrix, row_signs.astype(jnp.float32).reshape(rows // base, base), sylvester(base), padded)


def whole_exchange(matrix, row_signs, all_indices, scale):
    blocks = lax.axis_size("rows") * lax.axis_size("grp")
    row_dev, col_count = matrix.shape
    piece_rows = row_dev // blocks
    position = lax.axis_index(("rows", "grp"))
    signs = jnp.broadcast_to(row_signs.astype(jnp.float32)[:, None], (row_dev, TILE))
    before = local_transform(matrix, signs, min(256, row_dev))
    arrived = lax.all_to_all(
        before.reshape(blocks, piece_rows, col_count),
        ("rows", "grp"),
        split_axis=0,
        concat_axis=0,
        tiled=True,
    )
    first = jnp.arange(blocks, dtype=jnp.int32)[:, None] * row_dev + position * piece_rows
    within = all_indices - first
    hits = within[:, None, :] == jnp.arange(piece_rows, dtype=jnp.int32)[None, :, None]
    weights = jnp.max(hits.astype(jnp.float32), axis=2)
    weights = jnp.broadcast_to(weights[:, :, None], (blocks, piece_rows, TILE))
    half = gram_share(arrived, weights, scale)
    whole = (half + half.T) * 0.5
    pieces = []
    for i, count in enumerate(panel_tiles(col_count // TILE)[0]):
        row = whole[i * TILE : (i + 1) * TILE]
        tiles = [row[:, j * TILE : (j + 1) * TILE] for j in range(i, col_count // TILE)]
        tiles += [jnp.zeros((TILE, TILE), jnp.float32)] * (count - len(tiles))
        pieces += tiles
    return jnp.concatenate(pieces, axis=0)


def shards(matrix, row_signs, samples):
    count_rows = lax.axis_size("rows")
    blocks = count_rows * lax.axis_size("grp")
    row_dev, col_count = matrix.shape
    sample_dev = samples.shape[0]
    scale = (sample_dev * blocks) ** -0.5
    far = 4
    near = blocks // far
    chance = 1.0 - (1.0 - sample_dev / row_dev) ** far
    room = row_dev * chance + 5.0 * (row_dev * chance * (1.0 - chance)) ** 0.5
    room = min(row_dev, -(-int(room) // (16 * far)) * 16 * far)
    share_rows = col_count // count_rows

    def own(upper_factor):
        return lax.dynamic_slice_in_dim(upper_factor, lax.axis_index("rows") * share_rows, share_rows, 0)

    packed = exchange(matrix, row_signs, samples, near, far, room, scale)
    upper_factor, over = reduce_factor(packed, col_count)

    def again():
        all_indices = lax.all_gather(samples, ("rows", "grp"), axis=0)
        packed = whole_exchange(matrix, row_signs, all_indices, scale)
        return own(reduce_factor(packed, col_count)[0])

    return lax.cond(over[0, 0] > 0.0, again, lambda: own(upper_factor))


def solution(mesh):
    return jax.shard_map(
        shards,
        mesh=mesh,
        in_specs=(P(("rows", "grp"), None), P(("rows", "grp")), P(("rows", "grp"))),
        out_specs=P("rows", None),
        check_vma=False,
    )
```

```python
import functools

import jax
import jax.numpy as jnp
from jax import lax
from jax.experimental import pallas as pl
from jax.experimental.pallas import tpu as pltpu
from jax.sharding import PartitionSpec as P

MESH = pl.DeviceIdType.MESH
VMEM_LIMIT = 60 * 1024 * 1024
TILE = 128
AHEAD = 2


def sylvester(length):
    matrix = jnp.ones((1, 1), jnp.float32)
    while matrix.shape[0] < length:
        matrix = jnp.block([[matrix, matrix], [matrix, -matrix]])
    return matrix


def butterfly(parts):
    span = 1
    while span < len(parts):
        parts = list(parts)
        for start in range(0, len(parts), 2 * span):
            for i in range(start, start + span):
                low, high = parts[i], parts[i + span]
                parts[i], parts[i + span] = low + high, low - high
        span *= 2
    return parts


def split(x):
    high = x.astype(jnp.bfloat16)
    return high, (x - high.astype(jnp.float32)).astype(jnp.bfloat16)


def local_kernel(base, x_ref, s_ref, h_ref, o_ref):
    parts = []
    for i in range(x_ref.shape[0] // base):
        rows = slice(i * base, (i + 1) * base)
        high, low = split(x_ref[rows, :] * s_ref[rows, :])
        both = jnp.dot(h_ref[...], high, preferred_element_type=jnp.float32)
        both += jnp.dot(h_ref[...], low, preferred_element_type=jnp.float32)
        parts.append(both)
    for i, part in enumerate(butterfly(parts)):
        o_ref[i * base : (i + 1) * base, :] = part


def local_transform(matrix, signs, base):
    rows, cols = matrix.shape
    return pl.pallas_call(
        functools.partial(local_kernel, base),
        grid=(cols // TILE,),
        out_shape=jax.ShapeDtypeStruct((rows, cols), jnp.float32),
        in_specs=[
            pl.BlockSpec((rows, TILE), lambda c: (0, c)),
            pl.BlockSpec((rows, TILE), lambda c: (0, 0)),
            pl.BlockSpec((base, base), lambda c: (0, 0)),
        ],
        out_specs=pl.BlockSpec((rows, TILE), lambda c: (0, c)),
        compiler_params=pltpu.CompilerParams(vmem_limit_bytes=VMEM_LIMIT),
    )(matrix, signs, sylvester(base).astype(jnp.bfloat16))


def gram_kernel(scale, x_ref, w_ref, o_ref, left, right):
    blocks, step, cols = x_ref.shape
    rows = blocks * step

    @pl.when(pl.program_id(0) == 0)
    def _():
        o_ref[...] = jnp.zeros_like(o_ref)

    def mix(c, carry):
        at = pl.ds(pl.multiple_of(c * TILE, TILE), TILE)
        parts = butterfly([x_ref[b, :, at] for b in range(blocks)])
        for b in range(0, blocks, 2):
            x = jnp.concatenate(parts[b : b + 2], axis=0) * scale
            w = jnp.concatenate([w_ref[b], w_ref[b + 1]], axis=0)
            high, low = split(x)
            here = slice(b * step, (b + 2) * step)
            there = slice(rows + b * step, rows + (b + 2) * step)
            masked = (high.astype(jnp.float32) * w).astype(jnp.bfloat16)
            left[here, at] = masked
            right[here, at] = high
            left[there, at] = masked
            right[there, at] = (2.0 * low.astype(jnp.float32)).astype(jnp.bfloat16)
        return carry

    lax.fori_loop(0, cols // TILE, mix, 0)
    wide = 2 * TILE

    def add(n, carry):
        at = pl.ds(pl.multiple_of(n * wide, wide), wide)
        o_ref[:, at] += lax.dot_general(
            left[...], right[:, at], (((0,), (0,)), ((), ())), preferred_element_type=jnp.float32
        )
        return carry

    lax.fori_loop(0, cols // wide, add, 0)


def gram_share(arrived, weights, scale):
    blocks, piece, cols = arrived.shape
    step = 8
    return pl.pallas_call(
        functools.partial(gram_kernel, scale),
        grid=(piece // step,),
        out_shape=jax.ShapeDtypeStruct((cols, cols), jnp.float32),
        in_specs=[
            pl.BlockSpec((blocks, step, cols), lambda t: (0, t, 0)),
            pl.BlockSpec((blocks, step, TILE), lambda t: (0, t, 0)),
        ],
        out_specs=pl.BlockSpec((cols, cols), lambda t: (0, 0)),
        scratch_shapes=[pltpu.VMEM((2 * blocks * step, cols), jnp.bfloat16)] * 2,
        compiler_params=pltpu.CompilerParams(vmem_limit_bytes=VMEM_LIMIT),
    )(arrived, weights)


def panel_tiles(panels):
    sizes = [panels - i + (panels - i) % 2 for i in range(panels)]
    return sizes, [sum(sizes[:i]) for i in range(panels)]


def column_tiles(panels):
    sizes = [k + 1 + (k + 1) % 2 for k in range(panels)]
    return sizes, [sum(sizes[:k]) for k in range(panels)]


def segments(panels):
    sizes, starts = panel_tiles(panels)
    runs = [(0, 1), (1, 2), (2, 4), (4, panels)]
    return [(starts[i], sum(sizes[i:j])) for i, j in runs]


def dot3(a, b, dims):
    (ah, al), (bh, bl) = a, b
    go = functools.partial(lax.dot_general, dimension_numbers=(dims, ((), ())), preferred_element_type=jnp.float32)
    return go(ah, bh) + (go(ah, bl) + go(al, bh))

def spread(row):
    return jnp.broadcast_to(row, (8, TILE))

def factor_block(block, lines):
    count, group = TILE // 8, 4
    sub_id = lax.broadcasted_iota(jnp.int32, (8, TILE), 0)
    lane_id = lax.broadcasted_iota(jnp.int32, (8, TILE), 1)
    strips = [block[8 * i : 8 * i + 8, :] for i in range(count)]
    inverse = [(lane_id == sub_id + 8 * i).astype(jnp.float32) for i in range(count)]
    for first in range(0, count, group):
        last = first + group
        for s in range(first, last):
            columns = {
                i: [jnp.broadcast_to(strips[i][:, 8 * s + t : 8 * s + t + 1], (8, TILE)) for t in range(8)]
                for i in range(s, last)
            }
            for t in range(8):
                lines[s % 2, t] = columns[s][t]
            lines[s % 2, 8] = strips[s]
            lines[s % 2, 9] = inverse[s]
            pivot = {(r, t): spread(lines[s % 2, t, r : r + 1, :]) for t in range(8) for r in range(t, 8)}
            row = [spread(lines[s % 2, 8, q : q + 1, :]) for q in range(8)]
            inv_row = [spread(lines[s % 2, 9, q : q + 1, :]) for q in range(8)]
            for j in range(8):
                root = lax.rsqrt(pivot[j, j])
                for r in range(j + 1, 8):
                    pivot[r, j] = pivot[r, j] * root
                for t in range(j + 1, 8):
                    for r in range(t, 8):
                        pivot[r, t] = pivot[r, t] - pivot[r, j] * pivot[t, j]
                row[j] = row[j] * root
                inv_row[j] = inv_row[j] * root
                for r in range(j + 1, 8):
                    row[r] = row[r] - pivot[r, j] * row[j]
                    inv_row[r] = inv_row[r] - pivot[r, j] * inv_row[j]
                for i in range(s + 1, last):
                    left = columns[i]
                    left[j] = left[j] * root
                    for r in range(j + 1, 8):
                        left[r] = left[r] - pivot[r, j] * left[j]
                    strips[i] = strips[i] - left[j] * row[j]
                    inverse[i] = inverse[i] - left[j] * inv_row[j]
            for q in range(8):
                strips[s] = row[q] if q == 0 else jnp.where(sub_id == q, row[q], strips[s])
                inverse[s] = inv_row[q] if q == 0 else jnp.where(sub_id == q, inv_row[q], inverse[s])
        if last < count:
            high, low = split(jnp.concatenate(strips[first:last], axis=0))
            inv_high, inv_low = split(jnp.concatenate(inverse[first:last], axis=0))
            three = jnp.concatenate([high, low, high], axis=0)
            rest = jnp.concatenate([high, high, low], axis=0)
            inv_rest = jnp.concatenate([inv_high, inv_high, inv_low], axis=0)
            both = jnp.concatenate([rest, inv_rest], axis=1)
            change = lax.dot_general(three, both, (((0,), (0,)), ((), ())), preferred_element_type=jnp.float32)
            for i in range(last, count):
                strips[i] = strips[i] - change[8 * i : 8 * i + 8, :TILE]
                inverse[i] = inverse[i] - change[8 * i : 8 * i + 8, TILE:]
    return jnp.concatenate(inverse, axis=0)


def factor_panels(work, keep, lines, high, low):
    cols = work.shape[0]

    def panel(k, carry):
        base = pl.multiple_of(k * TILE, TILE)
        here = pl.ds(base, TILE)
        lower = split(factor_block(work[here, here], lines))
        wide_row = lax.broadcasted_iota(jnp.int32, (TILE, cols), 0) + base
        wide_lane = lax.broadcasted_iota(jnp.int32, (TILE, cols), 1)
        upper = dot3(lower, split(work[here, :]), ((1,), (0,)))
        upper = jnp.where(wide_lane >= wide_row, upper, 0.0)
        keep(k, upper)
        high[...], low[...] = split(upper)

        def trail(start, i, inner):
            there = pl.ds(pl.multiple_of(i * TILE, TILE), TILE)
            right = (high[:, start:], low[:, start:])
            work[there, start:] -= dot3((high[:, there], low[:, there]), right, ((0,), (0,)))
            return inner

        half = cols // TILE // 2
        lax.fori_loop(k + 1, half, functools.partial(trail, 0), 0)
        lax.fori_loop(jnp.maximum(k + 1, half), cols // TILE, functools.partial(trail, cols // 2), 0)
        return carry

    lax.fori_loop(0, cols // TILE, panel, 0)


def keep_all(u_ref):
    def keep(k, upper):
        u_ref[pl.ds(pl.multiple_of(k * TILE, TILE), TILE), :] = upper

    return keep


def unpack(source, work, panels):
    for i, start in enumerate(panel_tiles(panels)[1]):
        for j in range(i, panels):
            p = (start + j - i) * TILE
            work[i * TILE : (i + 1) * TILE, j * TILE : (j + 1) * TILE] = source[p : p + TILE, :]


def factor_kernel(g_ref, u_ref, over_ref, work, lines, high, low):
    over_ref[...] = g_ref[g_ref.shape[0] - 8 :, :]
    work[...] = jnp.zeros_like(work)
    unpack(g_ref, work, u_ref.shape[0] // TILE)
    factor_panels(work, keep_all(u_ref), lines, high, low)


def reduce_stages(groups, place, runs, g_ref, whole, in1, in2, in3, sum1, sum2, send, arrive):
    pair, plane, line = groups
    c, q, b, at = place
    started = []

    def copy_of(s, stage, t):
        first, n1, n2, n3 = sizes(s)
        near1, near2, near3 = first // pair, first // (pair * plane), first // (pair * plane * line)
        if stage == 0:
            other = (c + t) % pair
            source, target, peer = g_ref.at[rows(first + other * n1, n1)], in1.at[t - 1, rows(near1, n1)], at(other, q, b)
        elif stage == 1:
            other = (q + t) % plane
            source, target, peer = sum1.at[rows(near1 + other * n2, n2)], in2.at[t - 1, rows(near2, n2)], at(c, other, b)
        elif stage == 2:
            other = (b + t) % line
            source, target, peer = sum2.at[rows(near2 + other * n3, n3)], in3.at[t - 1, rows(near3, n3)], at(c, q, other)
        else:
            if stage == 3:
                here, peer = rows(first + c * n1 + q * n2 + b * n3, n3), at(c, q, (b + t) % line)
            elif stage == 4:
                here, peer = rows(first + c * n1 + q * n2, n2), at(c, (q + t) % plane, b)
            else:
                here, peer = rows(first + c * n1, n1), at((c + t) % pair, q, b)
            source, target = whole.at[here], whole.at[here]
        slot = stage * 4 + t
        return pltpu.make_async_remote_copy(
            src_ref=source,
            dst_ref=target,
            send_sem=send.at[s, slot],
            recv_sem=arrive.at[s, slot],
            device_id=peer,
            device_id_type=MESH,
        )

    counts = [pair, plane, line, line, plane, pair]

    def rows(first, count):
        return pl.ds(pl.multiple_of(first, 8), count)

    def sizes(s):
        first, tiles = runs[s]
        first, n1 = first * TILE, tiles * TILE
        return first, n1 // pair, n1 // (pair * plane), n1 // (pair * plane * line)

    def start(s, stage):
        for t in range(1, counts[stage]):
            copy_of(s, stage, t).start()
            started.append((s, stage, t))

    def arrived(s, stage):
        for t in range(1, counts[stage]):
            copy_of(s, stage, t).wait_recv()

    def scatter1(s):
        start(s, 0)

    def scatter2(s):
        first, n1, n2, n3 = sizes(s)
        mine = rows(first // pair, n1)
        arrived(s, 0)
        total = g_ref[rows(first + c * n1, n1), :]
        for t in range(1, pair):
            total = total + in1[t - 1, mine, :]
        sum1[mine, :] = total
        start(s, 1)

    def scatter3(s):
        first, n1, n2, n3 = sizes(s)
        mine = rows(first // (pair * plane), n2)
        arrived(s, 1)
        total = sum1[rows(first // pair + q * n2, n2), :]
        for t in range(1, plane):
            total = total + in2[t - 1, mine, :]
        sum2[mine, :] = total
        start(s, 2)

    def gather3(s):
        first, n1, n2, n3 = sizes(s)
        mine = rows(first // (pair * plane * line), n3)
        arrived(s, 2)
        total = sum2[rows(first // (pair * plane) + b * n3, n3), :]
        for t in range(1, line):
            total = total + in3[t - 1, mine, :]
        whole[rows(first + c * n1 + q * n2 + b * n3, n3), :] = total
        start(s, 3)

    def gather2(s):
        arrived(s, 3)
        start(s, 4)

    def gather1(s):
        arrived(s, 4)
        start(s, 5)

    def finish(s):
        arrived(s, 5)

    def drain():
        for item in started:
            copy_of(*item).wait_send()

    return [scatter1, scatter2, scatter3, gather3, gather2, gather1, finish], drain


def reduce_factor_kernel(
    groups, g_ref, u_ref, over_ref, whole, in1, in2, in3, sum1, sum2, send, arrive, work, lines, high, low
):
    pair, plane, line = groups
    width = lax.axis_size("grp")
    me = lax.axis_index("rows") * width + lax.axis_index("grp")
    c, q, b = me % pair, (me // pair) % plane, me // (pair * plane)

    def at(cc, qq, bb):
        index = (bb * plane + qq) * pair + cc
        return (index // width, index % width)

    peers = [at((c + t) % pair, q, b) for t in range(1, pair)]
    peers += [at(c, (q + t) % plane, b) for t in range(1, plane)]
    peers += [at(c, q, (b + t) % line) for t in range(1, line)]
    barrier = pltpu.get_barrier_semaphore()
    for peer in peers:
        pl.semaphore_signal(barrier, inc=1, device_id=peer, device_id_type=MESH)
    pl.semaphore_wait(barrier, len(peers))

    runs = segments(u_ref.shape[0] // TILE)
    stages, drain = reduce_stages(
        groups, (c, q, b, at), runs, g_ref, whole, in1, in2, in3, sum1, sum2, send, arrive
    )
    for step in range(len(runs) + len(stages) - 1):
        for k in reversed(range(len(stages))):
            if 0 <= step - k < len(runs):
                stages[k](step - k)
    drain()
    over_ref[...] = whole[whole.shape[0] - 8 :, :]
    unpack(whole, work, u_ref.shape[0] // TILE)
    factor_panels(work, keep_all(u_ref), lines, high, low)


def reduce_groups(tile_counts):
    devices = lax.axis_size("rows") * lax.axis_size("grp")
    pair, plane = 2, 4
    line = devices // (pair * plane)
    if devices % (pair * plane) or line != 4 or any(count * TILE % (8 * devices) for count in tile_counts):
        return None
    return pair, plane, line


def reduce_factor(packed, cols):
    devices = lax.axis_size("rows") * lax.axis_size("grp")
    rows = packed.shape[0]
    common = [
        pltpu.VMEM((cols, cols), jnp.float32),
        pltpu.VMEM((2, 10, 8, TILE), jnp.float32),
        pltpu.VMEM((TILE, cols), jnp.bfloat16),
        pltpu.VMEM((TILE, cols), jnp.bfloat16),
    ]
    call = functools.partial(
        pl.pallas_call,
        out_shape=[jax.ShapeDtypeStruct((cols, cols), jnp.float32), jax.ShapeDtypeStruct((8, TILE), jnp.float32)],
        in_specs=[pl.BlockSpec(memory_space=pltpu.VMEM)],
        out_specs=[pl.BlockSpec(memory_space=pltpu.VMEM)] * 2,
    )
    groups = reduce_groups([tiles for _, tiles in segments(cols // TILE)])
    if not groups:
        return call(
            factor_kernel,
            scratch_shapes=common,
            compiler_params=pltpu.CompilerParams(vmem_limit_bytes=VMEM_LIMIT),
        )(lax.psum(packed, ("rows", "grp")))
    pair, plane, line = groups
    runs = len(segments(cols // TILE))
    return call(
        functools.partial(reduce_factor_kernel, groups),
        scratch_shapes=[
            pltpu.VMEM((rows, TILE), jnp.float32),
            pltpu.VMEM((pair - 1, rows // pair, TILE), jnp.float32),
            pltpu.VMEM((plane - 1, rows // (pair * plane), TILE), jnp.float32),
            pltpu.VMEM((max(line - 1, 1), rows // devices, TILE), jnp.float32),
            pltpu.VMEM((rows // pair, TILE), jnp.float32),
            pltpu.VMEM((rows // (pair * plane), TILE), jnp.float32),
            pltpu.SemaphoreType.DMA((runs, 24)),
            pltpu.SemaphoreType.DMA((runs, 24)),
            *common,
        ],
        compiler_params=pltpu.CompilerParams(vmem_limit_bytes=VMEM_LIMIT, collective_id=1, has_side_effects=True),
    )(packed)


def exchange_kernel(
    sizes, scale, groups, x_ref, s_ref, h_ref, samples_ref, *refs
):
    if groups:
        out_ref, over_ref, g_ref, whole, in1, in2, in3, sum1, sum2, send, arrive, work, spare_lines, row_high, row_low, row_block = refs[:2] + refs[-14:]
        rest = refs[2:-14]
    else:
        g_ref, rest = refs[0], refs[1:]
    (x_in, signed_h, x_out, x_got, mixed, y_out, y_got, high, low, samples, taken, weights, pick_row, pick_ref,
    load, send_a, got_a, send_b, got_b, send_s, got_s) = rest
    near, far, ahead = sizes
    steps, rows = x_in.shape[0], x_in.shape[1]
    base, piece, share = h_ref.shape[0], rows // near, weights.shape[0] // far
    room = share * far
    width = lax.axis_size("grp")
    me = lax.axis_index("rows") * width + lax.axis_index("grp")
    a, b = me % near, me // near

    def at(aa, bb):
        index = bb * near + aa
        return (index // width, index % width)

    def loading(c):
        lanes = pl.ds(pl.multiple_of(c * TILE, TILE), TILE)
        return pltpu.make_async_copy(x_ref.at[:, lanes], x_in.at[c], load.at[c])

    def span(i, count):
        return pl.ds(pl.multiple_of(i * count, count), count)

    def near_copy(c, t):
        there = (a + t) % near
        return pltpu.make_async_remote_copy(
            src_ref=x_out.at[c, span(there, piece)],
            dst_ref=x_got.at[c, span(a, piece)],
            send_sem=send_a.at[c, t],
            recv_sem=got_a.at[c, t],
            device_id=at(there, b),
            device_id_type=MESH,
        )

    def far_copy(c, t):
        there = (b + t) % far
        return pltpu.make_async_remote_copy(
            src_ref=y_out.at[c, span(there, share)],
            dst_ref=y_got.at[c, span(b, share)],
            send_sem=send_b.at[c, t],
            recv_sem=got_b.at[c, t],
            device_id=at(a, there),
            device_id_type=MESH,
        )

    def each(first, last, act):
        def body(t, carry):
            act(t)
            return carry

        lax.fori_loop(first, last, body, 0)

    def picked(group, offset):
        return jnp.minimum(jnp.maximum(pick_ref[group, offset], 0), rows - 1)

    def sample_copy(t, along):
        there = at((a + t) % near, b) if along == 0 else at(a, (b + t) % far)
        source = samples_ref if along == 0 else samples.at[pl.ds(b * near, near)]
        target = samples.at[me] if along == 0 else samples.at[pl.ds(b * near, near)]
        return pltpu.make_async_remote_copy(
            src_ref=source,
            dst_ref=target,
            send_sem=send_s.at[along * near + t],
            recv_sem=got_s.at[along * near + t],
            device_id=there,
            device_id_type=MESH,
        )

    flag = TILE if groups else g_ref.shape[0] - 8

    def choose():
        lines = samples_ref.shape[0]
        position = lax.broadcasted_iota(jnp.int32, (piece, TILE), 0)
        ones = jnp.ones((TILE, TILE), jnp.bfloat16)

        def presence(kl):
            where = pl.ds(pl.multiple_of(kl * piece, piece), piece)
            for kz in range(far):
                block = kz * near + kl
                hits = jnp.zeros((piece, TILE), jnp.float32)
                for i in range(lines):
                    within = samples[block, i : i + 1, :] - (block * rows + a * piece)
                    hits += jnp.where(position == within, 1.0, 0.0)
                taken[kz, where, :] = jnp.dot(hits.astype(jnp.bfloat16), ones, preferred_element_type=jnp.float32)

        each(0, near, presence)
        row_id = lax.broadcasted_iota(jnp.int32, (TILE, TILE), 0)
        lane_id = lax.broadcasted_iota(jnp.int32, (TILE, TILE), 1)
        earlier = jnp.where(lane_id < row_id, 1.0, 0.0).astype(jnp.bfloat16)
        total = jnp.zeros((1, TILE), jnp.float32)
        for i in range(rows // TILE):
            here = slice(i * TILE, (i + 1) * TILE)
            need = taken[0, here, :]
            for kz in range(1, far):
                need = jnp.maximum(need, taken[kz, here, :])
            rank = jnp.dot(earlier, need.astype(jnp.bfloat16), preferred_element_type=jnp.float32)
            mixed[here, :] = jnp.where(need > 0.0, rank + total, -1.0)
            total = total + rank[TILE - 1 :, :] + need[TILE - 1 :, :]
        lane = lax.broadcasted_iota(jnp.int32, (8, TILE), 1).astype(jnp.float32)
        sub = lax.broadcasted_iota(jnp.int32, (8, TILE), 0).astype(jnp.float32)
        tiles = pick_row.shape[0]

        def find(r, found):
            for u in range(4):
                slot = mixed[pl.ds(pl.multiple_of(r * 32 + u * 8, 8), 8), :]
                number = sub + (r * 32 + u * 8).astype(jnp.float32)
                found = tuple(f + jnp.where(slot == lane + float(v * TILE), number, 0.0) for v, f in enumerate(found))
            return found

        found = lax.fori_loop(0, rows // 32, find, (jnp.zeros((8, TILE), jnp.float32),) * tiles)
        for v in range(tiles):
            pick_row[v : v + 1, :] = jnp.sum(found[v], axis=0, keepdims=True).astype(jnp.int32)
        copy = pltpu.make_async_copy(pick_row, pick_ref, load.at[steps])
        copy.start()
        copy.wait()

        def weigh(r):
            for u in range(8):
                place = b * share + r * 8 + u
                row = picked(place // TILE, place % TILE)
                for kz in range(far):
                    weights[pl.ds(pl.multiple_of(kz * share + r * 8, 8) + u, 1), :] = taken[kz, pl.ds(row, 1), :]

        each(0, share // 8, weigh)
        slot = lax.broadcasted_iota(jnp.int32, (share, TILE), 0) + b * share
        used = jnp.where(slot.astype(jnp.float32) < total, scale, 0.0)
        for kz in range(far):
            here = slice(kz * share, (kz + 1) * share)
            weights[here, :] = weights[here, :] * used
        g_ref[flag : flag + 8, :] = jnp.broadcast_to(jnp.where(total > float(room), 1.0, 0.0), (8, TILE))

    def transform(c):
        loading(c).wait()
        parts = []
        for i in range(rows // base):
            x_high, x_low = split(x_in[c, i * base : (i + 1) * base, :])
            part = jnp.dot(signed_h[i], x_high, preferred_element_type=jnp.float32)
            parts.append(part + jnp.dot(signed_h[i], x_low, preferred_element_type=jnp.float32))
        for i, part in enumerate(butterfly(parts)):
            x_out[c, i * base : (i + 1) * base, :] = part
        each(1, near, lambda t: near_copy(c, t).start())
        x_got[c, span(a, piece), :] = x_out[c, span(a, piece), :]

    def middle(c):
        each(1, near, lambda t: near_copy(c, t).wait_recv())
        block = min(32, piece)

        def mix(r):
            where = [pl.ds(pl.multiple_of(j * piece + r * block, block), block) for j in range(near)]
            for here, part in zip(where, butterfly([x_got[c, here, :] for here in where])):
                mixed[here, :] = part

        each(0, piece // block, mix)

        def keep(r):
            group, offset = (r * 32) // TILE, (r * 32) % TILE
            kept = [mixed[pl.ds(picked(group, offset + u), 1), :] for u in range(32)]
            for u in range(0, 32, 8):
                y_out[c, pl.ds(pl.multiple_of(r * 32 + u, 8), 8), :] = jnp.concatenate(kept[u : u + 8], axis=0)

        each(0, room // 32, keep)
        each(1, far, lambda t: far_copy(c, t).start())
        y_got[c, span(b, share), :] = y_out[c, span(b, share), :]

    def last(c):
        each(1, far, lambda t: far_copy(c, t).wait_recv())
        lanes = pl.ds(pl.multiple_of(c * TILE, TILE), TILE)

        def mix(r):
            where = [pl.ds(pl.multiple_of(j * share + r * 16, 16), 16) for j in range(far)]
            for here, part in zip(where, butterfly([y_got[c, here, :] for here in where])):
                x_high, x_low = split(part * weights[here, :])
                high[here, lanes] = x_high
                low[here, lanes] = x_low

        each(0, share // 16, mix)

        def gram(i):
            left = pl.ds(pl.multiple_of(i * TILE, TILE), TILE)
            if groups:
                half = c // 2
                first = 2 * half * (half + 1) + (c % 2) * (2 * half + 2) + 2 * i - c
            else:
                half = i // 2
                first = 2 * steps * half - 2 * half * (half - 1) + (i % 2) * (steps - 2 * half)
            tile = dot3((high[:, left], low[:, left]), (high[:, lanes], low[:, lanes]), ((0,), (0,)))
            g_ref[span(first + c - i, TILE), :] = tile

        each(0, c + 1, gram)

    each(0, steps, lambda c: loading(c).start())
    barrier = pltpu.get_barrier_semaphore()

    def greet(there):
        pl.semaphore_signal(barrier, inc=1, device_id=there, device_id_type=MESH)

    each(1, near, lambda t: greet(at((a + t) % near, b)))
    each(1, far, lambda t: greet(at(a, (b + t) % far)))
    for i in range(rows // base):
        signed_h[i] = (h_ref[...] * s_ref[i : i + 1, :]).astype(jnp.bfloat16)
    sizes_list, starts = column_tiles(steps) if groups else panel_tiles(steps)
    for i in range(0 if groups else 1, steps, 2):
        spare = (starts[i] + sizes_list[i] - 1) * TILE
        g_ref[spare : spare + TILE, :] = jnp.zeros((TILE, TILE), jnp.float32)
    samples[me] = samples_ref[...]
    pl.semaphore_wait(barrier, near + far - 2)
    each(1, near, lambda t: sample_copy(t, 0).start())
    transform(0)
    each(1, near, lambda t: sample_copy(t, 0).wait_recv())
    each(1, far, lambda t: sample_copy(t, 1).start())
    each(1, ahead, transform)
    each(1, far, lambda t: sample_copy(t, 1).wait_recv())
    choose()

    if groups:
        pair, plane, line = groups

        def place(cc, qq, bb):
            return at(qq * pair + cc, bb)

        runs = list(zip(starts, sizes_list))
        stages, drain = reduce_stages(
            groups, (a % pair, a // pair, b, place), runs, g_ref, whole, in1, in2, in3, sum1, sum2, send, arrive
        )

    def stage_at(j, stage, delay):
        for k in range(steps - delay + 1 if groups else 0):
            pl.when(j == k + delay)(functools.partial(stages[stage], k))

    def step(c):
        stage_at(c, 1, 2)

        @pl.when(c + ahead < steps)
        def _():
            transform(c + ahead)

        @pl.when(c < steps)
        def _():
            middle(c)

        stage_at(c, 2, 3)

        @pl.when(c > 0)
        def _():
            last(c - 1)

        stage_at(c, 0, 1)
        stage_at(c, 3, 4)

    each(0, steps + 1, step)
    if groups:
        for wave in range(6):
            for k in reversed(range(steps)):
                stage = min(steps - k, 4) + wave
                if stage < len(stages):
                    stages[stage](k)
        over_ref[...] = whole[flag : flag + 8, :]
        for k, start in enumerate(starts):
            for i in range(k + 1):
                tile = (start + i) * TILE
                work[i * TILE : (i + 1) * TILE, k * TILE : (k + 1) * TILE] = whole[tile : tile + TILE, :]
        drain()
        share_rows = out_ref.shape[0]
        own = lax.axis_index("rows") * share_rows

        def keep_own(k, upper):
            row_block[...] = upper

            @pl.when(own // TILE == k)
            def _():
                out_ref[...] = row_block[pl.ds(pl.multiple_of(own % TILE, 8), share_rows), :]

        factor_panels(work, keep_own, spare_lines, row_high, row_low)
    each(1, near, lambda t: sample_copy(t, 0).wait_send())
    each(1, far, lambda t: sample_copy(t, 1).wait_send())
    each(0, steps, lambda c: each(1, near, lambda t: near_copy(c, t).wait_send()))
    each(0, steps, lambda c: each(1, far, lambda t: far_copy(c, t).wait_send()))


def exchange(matrix, row_signs, samples, near, far, room, scale, groups):
    rows, cols = matrix.shape
    steps = cols // TILE
    base = min(256, rows)
    lines = -(-samples.shape[0] // TILE)
    padded = jnp.pad(samples, (0, lines * TILE - samples.shape[0]), constant_values=-1).reshape(lines, TILE)
    tiles = sum(panel_tiles(steps)[0])
    vmem = pl.BlockSpec(memory_space=pltpu.VMEM)
    picks = -(-room // TILE)
    packed = tiles * TILE
    gram = jax.ShapeDtypeStruct((packed, TILE), jnp.float32)
    fused = []
    if groups:
        pair, plane, line = groups
        share_rows = cols // lax.axis_size("rows")
        outs = [jax.ShapeDtypeStruct((share_rows, cols), jnp.float32), jax.ShapeDtypeStruct((8, TILE), jnp.float32)]
        fused = [
            pltpu.VMEM((packed, TILE), jnp.float32),
            pltpu.VMEM((packed, TILE), jnp.float32),
            pltpu.VMEM((pair - 1, packed // pair, TILE), jnp.float32),
            pltpu.VMEM((plane - 1, packed // (pair * plane), TILE), jnp.float32),
            pltpu.VMEM((max(line - 1, 1), packed // (near * far), TILE), jnp.float32),
            pltpu.VMEM((packed // pair, TILE), jnp.float32),
            pltpu.VMEM((packed // (pair * plane), TILE), jnp.float32),
            pltpu.SemaphoreType.DMA((steps, 24)),
            pltpu.SemaphoreType.DMA((steps, 24)),
            pltpu.VMEM((cols, cols), jnp.float32),
            pltpu.VMEM((2, 10, 8, TILE), jnp.float32),
            pltpu.VMEM((TILE, cols), jnp.bfloat16),
            pltpu.VMEM((TILE, cols), jnp.bfloat16),
            pltpu.VMEM((TILE, cols), jnp.float32),
        ]
    return pl.pallas_call(
        functools.partial(exchange_kernel, (near, far, min(AHEAD, steps)), scale, groups),
        out_shape=outs if groups else gram,
        in_specs=[pl.BlockSpec(memory_space=pl.ANY), vmem, vmem, vmem],
        out_specs=[vmem, vmem] if groups else vmem,
        scratch_shapes=[
            pltpu.VMEM((steps, rows, TILE), jnp.float32),
            pltpu.VMEM((rows // base, base, base), jnp.bfloat16),
            pltpu.VMEM((steps, rows, TILE), jnp.float32),
            pltpu.VMEM((steps, rows, TILE), jnp.float32),
            pltpu.VMEM((rows, TILE), jnp.float32),
            pltpu.VMEM((steps, room, TILE), jnp.float32),
            pltpu.VMEM((steps, room, TILE), jnp.float32),
            pltpu.VMEM((room, cols), jnp.bfloat16),
            pltpu.VMEM((room, cols), jnp.bfloat16),
            pltpu.VMEM((near * far, lines, TILE), jnp.int32),
            pltpu.VMEM((far, rows, TILE), jnp.float32),
            pltpu.VMEM((room, TILE), jnp.float32),
            pltpu.VMEM((picks, TILE), jnp.int32),
            pltpu.SMEM((picks, TILE), jnp.int32),
            pltpu.SemaphoreType.DMA((steps + 1,)),
            pltpu.SemaphoreType.DMA((steps, near)),
            pltpu.SemaphoreType.DMA((steps, near)),
            pltpu.SemaphoreType.DMA((steps, far)),
            pltpu.SemaphoreType.DMA((steps, far)),
            pltpu.SemaphoreType.DMA((near + far,)),
            pltpu.SemaphoreType.DMA((near + far,)),
            *fused,
        ],
        compiler_params=pltpu.CompilerParams(vmem_limit_bytes=VMEM_LIMIT, collective_id=2, has_side_effects=True),
    )(matrix, row_signs.astype(jnp.float32).reshape(rows // base, base), sylvester(base), padded)


def whole_exchange(matrix, row_signs, all_indices, scale):
    blocks = lax.axis_size("rows") * lax.axis_size("grp")
    row_dev, col_count = matrix.shape
    piece_rows = row_dev // blocks
    position = lax.axis_index(("rows", "grp"))
    signs = jnp.broadcast_to(row_signs.astype(jnp.float32)[:, None], (row_dev, TILE))
    before = local_transform(matrix, signs, min(256, row_dev))
    arrived = lax.all_to_all(
        before.reshape(blocks, piece_rows, col_count),
        ("rows", "grp"),
        split_axis=0,
        concat_axis=0,
        tiled=True,
    )
    first = jnp.arange(blocks, dtype=jnp.int32)[:, None] * row_dev + position * piece_rows
    within = all_indices - first
    hits = within[:, None, :] == jnp.arange(piece_rows, dtype=jnp.int32)[None, :, None]
    weights = jnp.max(hits.astype(jnp.float32), axis=2)
    weights = jnp.broadcast_to(weights[:, :, None], (blocks, piece_rows, TILE))
    half = gram_share(arrived, weights, scale)
    whole = (half + half.T) * 0.5
    pieces = []
    for i, count in enumerate(panel_tiles(col_count // TILE)[0]):
        row = whole[i * TILE : (i + 1) * TILE]
        tiles = [row[:, j * TILE : (j + 1) * TILE] for j in range(i, col_count // TILE)]
        tiles += [jnp.zeros((TILE, TILE), jnp.float32)] * (count - len(tiles))
        pieces += tiles
    return jnp.concatenate(pieces, axis=0)


def shards(matrix, row_signs, samples):
    count_rows = lax.axis_size("rows")
    blocks = count_rows * lax.axis_size("grp")
    row_dev, col_count = matrix.shape
    sample_dev = samples.shape[0]
    scale = (sample_dev * blocks) ** -0.5
    far = 4
    near = blocks // far
    chance = 1.0 - (1.0 - sample_dev / row_dev) ** far
    room = row_dev * chance + 5.0 * (row_dev * chance * (1.0 - chance)) ** 0.5
    room = min(row_dev, -(-int(room) // (16 * far)) * 16 * far)
    share_rows = col_count // count_rows

    def own(upper_factor):
        return lax.dynamic_slice_in_dim(upper_factor, lax.axis_index("rows") * share_rows, share_rows, 0)

    groups = reduce_groups([tiles for tiles in column_tiles(col_count // TILE)[0]])
    if groups:
        mine, over = exchange(matrix, row_signs, samples, near, far, room, scale, groups)
    else:
        packed = exchange(matrix, row_signs, samples, near, far, room, scale, None)
        upper_factor, over = reduce_factor(packed, col_count)
        mine = own(upper_factor)

    def again():
        all_indices = lax.all_gather(samples, ("rows", "grp"), axis=0)
        packed = whole_exchange(matrix, row_signs, all_indices, scale)
        return own(reduce_factor(packed, col_count)[0])

    return lax.cond(over[0, 0] > 0.0, again, lambda: mine)


def solution(mesh):
    return jax.shard_map(
        shards,
        mesh=mesh,
        in_specs=(P(("rows", "grp"), None), P(("rows", "grp")), P(("rows", "grp"))),
        out_specs=P("rows", None),
        check_vma=False,
    )
```

```python
import functools

import jax
import jax.numpy as jnp
from jax import lax
from jax.experimental import pallas as pl
from jax.experimental.pallas import tpu as pltpu
from jax.sharding import PartitionSpec as P

MESH = pl.DeviceIdType.MESH
VMEM_LIMIT = 60 * 1024 * 1024
TILE = 128
AHEAD = 2


def sylvester(length):
    matrix = jnp.ones((1, 1), jnp.float32)
    while matrix.shape[0] < length:
        matrix = jnp.block([[matrix, matrix], [matrix, -matrix]])
    return matrix


def butterfly(parts):
    span = 1
    while span < len(parts):
        parts = list(parts)
        for start in range(0, len(parts), 2 * span):
            for i in range(start, start + span):
                low, high = parts[i], parts[i + span]
                parts[i], parts[i + span] = low + high, low - high
        span *= 2
    return parts


def split(x):
    high = x.astype(jnp.bfloat16)
    return high, (x - high.astype(jnp.float32)).astype(jnp.bfloat16)


def local_kernel(base, x_ref, s_ref, h_ref, o_ref):
    parts = []
    for i in range(x_ref.shape[0] // base):
        rows = slice(i * base, (i + 1) * base)
        high, low = split(x_ref[rows, :] * s_ref[rows, :])
        both = jnp.dot(h_ref[...], high, preferred_element_type=jnp.float32)
        both += jnp.dot(h_ref[...], low, preferred_element_type=jnp.float32)
        parts.append(both)
    for i, part in enumerate(butterfly(parts)):
        o_ref[i * base : (i + 1) * base, :] = part


def local_transform(matrix, signs, base):
    rows, cols = matrix.shape
    return pl.pallas_call(
        functools.partial(local_kernel, base),
        grid=(cols // TILE,),
        out_shape=jax.ShapeDtypeStruct((rows, cols), jnp.float32),
        in_specs=[
            pl.BlockSpec((rows, TILE), lambda c: (0, c)),
            pl.BlockSpec((rows, TILE), lambda c: (0, 0)),
            pl.BlockSpec((base, base), lambda c: (0, 0)),
        ],
        out_specs=pl.BlockSpec((rows, TILE), lambda c: (0, c)),
        compiler_params=pltpu.CompilerParams(vmem_limit_bytes=VMEM_LIMIT),
    )(matrix, signs, sylvester(base).astype(jnp.bfloat16))


def gram_kernel(scale, x_ref, w_ref, o_ref, left, right):
    blocks, step, cols = x_ref.shape
    rows = blocks * step

    @pl.when(pl.program_id(0) == 0)
    def _():
        o_ref[...] = jnp.zeros_like(o_ref)

    def mix(c, carry):
        at = pl.ds(pl.multiple_of(c * TILE, TILE), TILE)
        parts = butterfly([x_ref[b, :, at] for b in range(blocks)])
        for b in range(0, blocks, 2):
            x = jnp.concatenate(parts[b : b + 2], axis=0) * scale
            w = jnp.concatenate([w_ref[b], w_ref[b + 1]], axis=0)
            high, low = split(x)
            here = slice(b * step, (b + 2) * step)
            there = slice(rows + b * step, rows + (b + 2) * step)
            masked = (high.astype(jnp.float32) * w).astype(jnp.bfloat16)
            left[here, at] = masked
            right[here, at] = high
            left[there, at] = masked
            right[there, at] = (2.0 * low.astype(jnp.float32)).astype(jnp.bfloat16)
        return carry

    lax.fori_loop(0, cols // TILE, mix, 0)
    wide = 2 * TILE

    def add(n, carry):
        at = pl.ds(pl.multiple_of(n * wide, wide), wide)
        o_ref[:, at] += lax.dot_general(
            left[...], right[:, at], (((0,), (0,)), ((), ())), preferred_element_type=jnp.float32
        )
        return carry

    lax.fori_loop(0, cols // wide, add, 0)


def gram_share(arrived, weights, scale):
    blocks, piece, cols = arrived.shape
    step = 8
    return pl.pallas_call(
        functools.partial(gram_kernel, scale),
        grid=(piece // step,),
        out_shape=jax.ShapeDtypeStruct((cols, cols), jnp.float32),
        in_specs=[
            pl.BlockSpec((blocks, step, cols), lambda t: (0, t, 0)),
            pl.BlockSpec((blocks, step, TILE), lambda t: (0, t, 0)),
        ],
        out_specs=pl.BlockSpec((cols, cols), lambda t: (0, 0)),
        scratch_shapes=[pltpu.VMEM((2 * blocks * step, cols), jnp.bfloat16)] * 2,
        compiler_params=pltpu.CompilerParams(vmem_limit_bytes=VMEM_LIMIT),
    )(arrived, weights)


def panel_tiles(panels):
    sizes = [panels - i + (panels - i) % 2 for i in range(panels)]
    return sizes, [sum(sizes[:i]) for i in range(panels)]


def column_tiles(panels):
    sizes = [k + 1 + (k + 1) % 2 for k in range(panels)]
    return sizes, [sum(sizes[:k]) for k in range(panels)]


def segments(panels):
    sizes, starts = panel_tiles(panels)
    runs = [(0, 1), (1, 2), (2, 4), (4, panels)]
    return [(starts[i], sum(sizes[i:j])) for i, j in runs]


def dot3(a, b, dims):
    (ah, al), (bh, bl) = a, b
    go = functools.partial(lax.dot_general, dimension_numbers=(dims, ((), ())), preferred_element_type=jnp.float32)
    return go(ah, bh) + (go(ah, bl) + go(al, bh))

def spread(row):
    return jnp.broadcast_to(row, (8, TILE))

def factor_block(block, lines):
    count, group = TILE // 8, 8
    sub_id = lax.broadcasted_iota(jnp.int32, (8, TILE), 0)
    lane_id = lax.broadcasted_iota(jnp.int32, (8, TILE), 1)
    strips = [block[8 * i : 8 * i + 8, :] for i in range(count)]
    inverse = [(lane_id == sub_id + 8 * i).astype(jnp.float32) for i in range(count)]
    for first in range(0, count, group):
        last = first + group
        for s in range(first, last):
            columns = {
                i: [jnp.broadcast_to(strips[i][:, 8 * s + t : 8 * s + t + 1], (8, TILE)) for t in range(8)]
                for i in range(s, last)
            }
            for t in range(8):
                lines[s % 2, t] = columns[s][t]
            lines[s % 2, 8] = strips[s]
            lines[s % 2, 9] = inverse[s]
            pivot = {(r, t): spread(lines[s % 2, t, r : r + 1, :]) for t in range(8) for r in range(t, 8)}
            row = [spread(lines[s % 2, 8, q : q + 1, :]) for q in range(8)]
            inv_row = [spread(lines[s % 2, 9, q : q + 1, :]) for q in range(8)]
            for j in range(8):
                root = lax.rsqrt(pivot[j, j])
                for r in range(j + 1, 8):
                    pivot[r, j] = pivot[r, j] * root
                for t in range(j + 1, 8):
                    for r in range(t, 8):
                        pivot[r, t] = pivot[r, t] - pivot[r, j] * pivot[t, j]
                row[j] = row[j] * root
                inv_row[j] = inv_row[j] * root
                for r in range(j + 1, 8):
                    row[r] = row[r] - pivot[r, j] * row[j]
                    inv_row[r] = inv_row[r] - pivot[r, j] * inv_row[j]
                for i in range(s + 1, last):
                    left = columns[i]
                    left[j] = left[j] * root
                    for r in range(j + 1, 8):
                        left[r] = left[r] - pivot[r, j] * left[j]
                    strips[i] = strips[i] - left[j] * row[j]
                    inverse[i] = inverse[i] - left[j] * inv_row[j]
            for q in range(8):
                strips[s] = row[q] if q == 0 else jnp.where(sub_id == q, row[q], strips[s])
                inverse[s] = inv_row[q] if q == 0 else jnp.where(sub_id == q, inv_row[q], inverse[s])
        if last < count:
            high, low = split(jnp.concatenate(strips[first:last], axis=0))
            inv_high, inv_low = split(jnp.concatenate(inverse[first:last], axis=0))
            three = jnp.concatenate([high, low, high], axis=0)
            rest = jnp.concatenate([high, high, low], axis=0)
            inv_rest = jnp.concatenate([inv_high, inv_high, inv_low], axis=0)
            both = jnp.concatenate([rest, inv_rest], axis=1)
            change = lax.dot_general(three, both, (((0,), (0,)), ((), ())), preferred_element_type=jnp.float32)
            for i in range(last, count):
                strips[i] = strips[i] - change[8 * i : 8 * i + 8, :TILE]
                inverse[i] = inverse[i] - change[8 * i : 8 * i + 8, TILE:]
    return jnp.concatenate(inverse, axis=0)


def factor_panels(work, keep, lines, high, low):
    cols = work.shape[0]

    def panel(k, carry):
        base = pl.multiple_of(k * TILE, TILE)
        here = pl.ds(base, TILE)
        lower = split(factor_block(work[here, here], lines))
        wide_row = lax.broadcasted_iota(jnp.int32, (TILE, cols), 0) + base
        wide_lane = lax.broadcasted_iota(jnp.int32, (TILE, cols), 1)
        work_high, work_low = split(work[here, :])
        left = jnp.concatenate([lower[0], lower[1], lower[0]], axis=1)
        right = jnp.concatenate([work_high, work_high, work_low], axis=0)
        upper = jnp.dot(left, right, preferred_element_type=jnp.float32)
        upper = jnp.where(wide_lane >= wide_row, upper, 0.0)
        keep(k, upper)
        high[...], low[...] = split(upper)

        def trail(start, i, inner):
            there = pl.ds(pl.multiple_of(i * TILE, TILE), TILE)
            left = jnp.concatenate([high[:, there], low[:, there], high[:, there]], axis=0)
            right = jnp.concatenate([high[:, start:], high[:, start:], low[:, start:]], axis=0)
            work[there, start:] -= lax.dot_general(left, right, (((0,), (0,)), ((), ())), preferred_element_type=jnp.float32)
            return inner

        for part in range(4):
            first, end = part * cols // TILE // 4, (part + 1) * cols // TILE // 4
            lax.fori_loop(jnp.maximum(k + 1, first), end, functools.partial(trail, first * TILE), 0)
        return carry

    lax.fori_loop(0, cols // TILE, panel, 0)


def keep_all(u_ref):
    def keep(k, upper):
        u_ref[pl.ds(pl.multiple_of(k * TILE, TILE), TILE), :] = upper

    return keep


def unpack(source, work, panels):
    for i, start in enumerate(panel_tiles(panels)[1]):
        for j in range(i, panels):
            p = (start + j - i) * TILE
            work[i * TILE : (i + 1) * TILE, j * TILE : (j + 1) * TILE] = source[p : p + TILE, :]


def factor_kernel(g_ref, u_ref, over_ref, work, lines, high, low):
    over_ref[...] = g_ref[g_ref.shape[0] - 8 :, :]
    work[...] = jnp.zeros_like(work)
    unpack(g_ref, work, u_ref.shape[0] // TILE)
    factor_panels(work, keep_all(u_ref), lines, high, low)


def reduce_stages(groups, place, runs, g_ref, whole, in1, in2, in3, sum1, sum2, send, arrive):
    pair, plane, line = groups
    c, q, b, at = place
    started = []

    def copy_of(s, stage, t):
        first, n1, n2, n3 = sizes(s)
        near1, near2, near3 = first // pair, first // (pair * plane), first // (pair * plane * line)
        if stage == 0:
            other = (c + t) % pair
            source, target, peer = g_ref.at[rows(first + other * n1, n1)], in1.at[t - 1, rows(near1, n1)], at(other, q, b)
        elif stage == 1:
            other = (q + t) % plane
            source, target, peer = sum1.at[rows(near1 + other * n2, n2)], in2.at[t - 1, rows(near2, n2)], at(c, other, b)
        elif stage == 2:
            other = (b + t) % line
            source, target, peer = sum2.at[rows(near2 + other * n3, n3)], in3.at[t - 1, rows(near3, n3)], at(c, q, other)
        else:
            if stage == 3:
                here, peer = rows(first + c * n1 + q * n2 + b * n3, n3), at(c, q, (b + t) % line)
            elif stage == 4:
                here, peer = rows(first + c * n1 + q * n2, n2), at(c, (q + t) % plane, b)
            else:
                here, peer = rows(first + c * n1, n1), at((c + t) % pair, q, b)
            source, target = whole.at[here], whole.at[here]
        slot = stage * 4 + t
        return pltpu.make_async_remote_copy(
            src_ref=source,
            dst_ref=target,
            send_sem=send.at[s, slot],
            recv_sem=arrive.at[s, slot],
            device_id=peer,
            device_id_type=MESH,
        )

    counts = [pair, plane, line, line, plane, pair]

    def rows(first, count):
        return pl.ds(pl.multiple_of(first, 8), count)

    def sizes(s):
        first, tiles = runs[s]
        first, n1 = first * TILE, tiles * TILE
        return first, n1 // pair, n1 // (pair * plane), n1 // (pair * plane * line)

    def start(s, stage):
        for t in range(1, counts[stage]):
            copy_of(s, stage, t).start()
            started.append((s, stage, t))

    def arrived(s, stage):
        for t in range(1, counts[stage]):
            copy_of(s, stage, t).wait_recv()

    def scatter1(s):
        start(s, 0)

    def scatter2(s):
        first, n1, n2, n3 = sizes(s)
        mine = rows(first // pair, n1)
        arrived(s, 0)
        total = g_ref[rows(first + c * n1, n1), :]
        for t in range(1, pair):
            total = total + in1[t - 1, mine, :]
        sum1[mine, :] = total
        start(s, 1)

    def scatter3(s):
        first, n1, n2, n3 = sizes(s)
        mine = rows(first // (pair * plane), n2)
        arrived(s, 1)
        total = sum1[rows(first // pair + q * n2, n2), :]
        for t in range(1, plane):
            total = total + in2[t - 1, mine, :]
        sum2[mine, :] = total
        start(s, 2)

    def gather3(s):
        first, n1, n2, n3 = sizes(s)
        mine = rows(first // (pair * plane * line), n3)
        arrived(s, 2)
        total = sum2[rows(first // (pair * plane) + b * n3, n3), :]
        for t in range(1, line):
            total = total + in3[t - 1, mine, :]
        whole[rows(first + c * n1 + q * n2 + b * n3, n3), :] = total
        start(s, 3)

    def gather2(s):
        arrived(s, 3)
        start(s, 4)

    def gather1(s):
        arrived(s, 4)
        start(s, 5)

    def finish(s):
        arrived(s, 5)

    def drain():
        for item in started:
            copy_of(*item).wait_send()

    return [scatter1, scatter2, scatter3, gather3, gather2, gather1, finish], drain


def reduce_factor_kernel(
    groups, g_ref, u_ref, over_ref, whole, in1, in2, in3, sum1, sum2, send, arrive, work, lines, high, low
):
    pair, plane, line = groups
    width = lax.axis_size("grp")
    me = lax.axis_index("rows") * width + lax.axis_index("grp")
    c, q, b = me % pair, (me // pair) % plane, me // (pair * plane)

    def at(cc, qq, bb):
        index = (bb * plane + qq) * pair + cc
        return (index // width, index % width)

    peers = [at((c + t) % pair, q, b) for t in range(1, pair)]
    peers += [at(c, (q + t) % plane, b) for t in range(1, plane)]
    peers += [at(c, q, (b + t) % line) for t in range(1, line)]
    barrier = pltpu.get_barrier_semaphore()
    for peer in peers:
        pl.semaphore_signal(barrier, inc=1, device_id=peer, device_id_type=MESH)
    pl.semaphore_wait(barrier, len(peers))

    runs = segments(u_ref.shape[0] // TILE)
    stages, drain = reduce_stages(
        groups, (c, q, b, at), runs, g_ref, whole, in1, in2, in3, sum1, sum2, send, arrive
    )
    for step in range(len(runs) + len(stages) - 1):
        for k in reversed(range(len(stages))):
            if 0 <= step - k < len(runs):
                stages[k](step - k)
    drain()
    over_ref[...] = whole[whole.shape[0] - 8 :, :]
    unpack(whole, work, u_ref.shape[0] // TILE)
    factor_panels(work, keep_all(u_ref), lines, high, low)


def reduce_groups(tile_counts):
    devices = lax.axis_size("rows") * lax.axis_size("grp")
    pair, plane = 2, 4
    line = devices // (pair * plane)
    if devices % (pair * plane) or line != 4 or any(count * TILE % (8 * devices) for count in tile_counts):
        return None
    return pair, plane, line


def reduce_factor(packed, cols):
    devices = lax.axis_size("rows") * lax.axis_size("grp")
    rows = packed.shape[0]
    common = [
        pltpu.VMEM((cols, cols), jnp.float32),
        pltpu.VMEM((2, 10, 8, TILE), jnp.float32),
        pltpu.VMEM((TILE, cols), jnp.bfloat16),
        pltpu.VMEM((TILE, cols), jnp.bfloat16),
    ]
    call = functools.partial(
        pl.pallas_call,
        out_shape=[jax.ShapeDtypeStruct((cols, cols), jnp.float32), jax.ShapeDtypeStruct((8, TILE), jnp.float32)],
        in_specs=[pl.BlockSpec(memory_space=pltpu.VMEM)],
        out_specs=[pl.BlockSpec(memory_space=pltpu.VMEM)] * 2,
    )
    groups = reduce_groups([tiles for _, tiles in segments(cols // TILE)])
    if not groups:
        return call(
            factor_kernel,
            scratch_shapes=common,
            compiler_params=pltpu.CompilerParams(vmem_limit_bytes=VMEM_LIMIT),
        )(lax.psum(packed, ("rows", "grp")))
    pair, plane, line = groups
    runs = len(segments(cols // TILE))
    return call(
        functools.partial(reduce_factor_kernel, groups),
        scratch_shapes=[
            pltpu.VMEM((rows, TILE), jnp.float32),
            pltpu.VMEM((pair - 1, rows // pair, TILE), jnp.float32),
            pltpu.VMEM((plane - 1, rows // (pair * plane), TILE), jnp.float32),
            pltpu.VMEM((max(line - 1, 1), rows // devices, TILE), jnp.float32),
            pltpu.VMEM((rows // pair, TILE), jnp.float32),
            pltpu.VMEM((rows // (pair * plane), TILE), jnp.float32),
            pltpu.SemaphoreType.DMA((runs, 24)),
            pltpu.SemaphoreType.DMA((runs, 24)),
            *common,
        ],
        compiler_params=pltpu.CompilerParams(vmem_limit_bytes=VMEM_LIMIT, collective_id=1, has_side_effects=True),
    )(packed)


def exchange_kernel(
    sizes, scale, groups, x_ref, s_ref, h_ref, samples_ref, *refs
):
    if groups:
        out_ref, over_ref, g_ref, whole, in1, in2, in3, sum1, sum2, send, arrive, work, spare_lines, row_high, row_low, row_block = refs[:2] + refs[-14:]
        rest = refs[2:-14]
    else:
        g_ref, rest = refs[0], refs[1:]
    (x_in, signed_h, x_out, x_got, mixed, y_out, y_got, high, low, samples, taken, weights, pick_row, pick_ref,
    load, send_a, got_a, send_b, got_b, send_s, got_s) = rest
    near, far, ahead = sizes
    steps, rows = x_in.shape[0], x_in.shape[1]
    base, piece, share = h_ref.shape[0], rows // near, weights.shape[0] // far
    room = share * far
    width = lax.axis_size("grp")
    me = lax.axis_index("rows") * width + lax.axis_index("grp")
    a, b = me % near, me // near

    def at(aa, bb):
        index = bb * near + aa
        return (index // width, index % width)

    def loading(c):
        lanes = pl.ds(pl.multiple_of(c * TILE, TILE), TILE)
        return pltpu.make_async_copy(x_ref.at[:, lanes], x_in.at[c], load.at[c])

    def span(i, count):
        return pl.ds(pl.multiple_of(i * count, count), count)

    def near_copy(c, t):
        there = (a + t) % near
        return pltpu.make_async_remote_copy(
            src_ref=x_out.at[c, span(there, piece)],
            dst_ref=x_got.at[c, span(a, piece)],
            send_sem=send_a.at[c, t],
            recv_sem=got_a.at[c, t],
            device_id=at(there, b),
            device_id_type=MESH,
        )

    def far_copy(c, t):
        there = (b + t) % far
        return pltpu.make_async_remote_copy(
            src_ref=y_out.at[c, span(there, share)],
            dst_ref=y_got.at[c, span(b, share)],
            send_sem=send_b.at[c, t],
            recv_sem=got_b.at[c, t],
            device_id=at(a, there),
            device_id_type=MESH,
        )

    def each(first, last, act):
        def body(t, carry):
            act(t)
            return carry

        lax.fori_loop(first, last, body, 0)

    def picked(group, offset):
        return jnp.minimum(jnp.maximum(pick_ref[group, offset], 0), rows - 1)

    def sample_copy(t, along):
        there = at((a + t) % near, b) if along == 0 else at(a, (b + t) % far)
        source = samples_ref if along == 0 else samples.at[pl.ds(b * near, near)]
        target = samples.at[me] if along == 0 else samples.at[pl.ds(b * near, near)]
        return pltpu.make_async_remote_copy(
            src_ref=source,
            dst_ref=target,
            send_sem=send_s.at[along * near + t],
            recv_sem=got_s.at[along * near + t],
            device_id=there,
            device_id_type=MESH,
        )

    flag = TILE if groups else g_ref.shape[0] - 8

    def choose():
        lines = samples_ref.shape[0]
        position = lax.broadcasted_iota(jnp.int32, (piece, TILE), 0)
        ones = jnp.ones((TILE, TILE), jnp.bfloat16)

        def presence(kl):
            where = pl.ds(pl.multiple_of(kl * piece, piece), piece)
            for kz in range(far):
                block = kz * near + kl
                hits = jnp.zeros((piece, TILE), jnp.float32)
                for i in range(lines):
                    within = samples[block, i : i + 1, :] - (block * rows + a * piece)
                    hits += jnp.where(position == within, 1.0, 0.0)
                taken[kz, where, :] = jnp.dot(hits.astype(jnp.bfloat16), ones, preferred_element_type=jnp.float32)

        each(0, near, presence)
        row_id = lax.broadcasted_iota(jnp.int32, (TILE, TILE), 0)
        lane_id = lax.broadcasted_iota(jnp.int32, (TILE, TILE), 1)
        earlier = jnp.where(lane_id < row_id, 1.0, 0.0).astype(jnp.bfloat16)
        total = jnp.zeros((1, TILE), jnp.float32)
        for i in range(rows // TILE):
            here = slice(i * TILE, (i + 1) * TILE)
            need = taken[0, here, :]
            for kz in range(1, far):
                need = jnp.maximum(need, taken[kz, here, :])
            rank = jnp.dot(earlier, need.astype(jnp.bfloat16), preferred_element_type=jnp.float32)
            mixed[here, :] = jnp.where(need > 0.0, rank + total, -1.0)
            total = total + rank[TILE - 1 :, :] + need[TILE - 1 :, :]
        lane = lax.broadcasted_iota(jnp.int32, (8, TILE), 1).astype(jnp.float32)
        sub = lax.broadcasted_iota(jnp.int32, (8, TILE), 0).astype(jnp.float32)
        tiles = pick_row.shape[0]

        def find(r, found):
            for u in range(4):
                slot = mixed[pl.ds(pl.multiple_of(r * 32 + u * 8, 8), 8), :]
                number = sub + (r * 32 + u * 8).astype(jnp.float32)
                found = tuple(f + jnp.where(slot == lane + float(v * TILE), number, 0.0) for v, f in enumerate(found))
            return found

        found = lax.fori_loop(0, rows // 32, find, (jnp.zeros((8, TILE), jnp.float32),) * tiles)
        for v in range(tiles):
            pick_row[v : v + 1, :] = jnp.sum(found[v], axis=0, keepdims=True).astype(jnp.int32)
        copy = pltpu.make_async_copy(pick_row, pick_ref, load.at[steps])
        copy.start()
        copy.wait()

        def weigh(r):
            for u in range(8):
                place = b * share + r * 8 + u
                row = picked(place // TILE, place % TILE)
                for kz in range(far):
                    weights[pl.ds(pl.multiple_of(kz * share + r * 8, 8) + u, 1), :] = taken[kz, pl.ds(row, 1), :]

        each(0, share // 8, weigh)
        slot = lax.broadcasted_iota(jnp.int32, (share, TILE), 0) + b * share
        used = jnp.where(slot.astype(jnp.float32) < total, scale, 0.0)
        for kz in range(far):
            here = slice(kz * share, (kz + 1) * share)
            weights[here, :] = weights[here, :] * used
        g_ref[flag : flag + 8, :] = jnp.broadcast_to(jnp.where(total > float(room), 1.0, 0.0), (8, TILE))

    def transform(c):
        loading(c).wait()
        parts = []
        for i in range(rows // base):
            x_high, x_low = split(x_in[c, i * base : (i + 1) * base, :])
            part = jnp.dot(signed_h[i], x_high, preferred_element_type=jnp.float32)
            parts.append(part + jnp.dot(signed_h[i], x_low, preferred_element_type=jnp.float32))
        for i, part in enumerate(butterfly(parts)):
            x_out[c, i * base : (i + 1) * base, :] = part
        each(1, near, lambda t: near_copy(c, t).start())
        x_got[c, span(a, piece), :] = x_out[c, span(a, piece), :]

    def middle(c):
        each(1, near, lambda t: near_copy(c, t).wait_recv())
        block = min(32, piece)

        def mix(r):
            where = [pl.ds(pl.multiple_of(j * piece + r * block, block), block) for j in range(near)]
            for here, part in zip(where, butterfly([x_got[c, here, :] for here in where])):
                mixed[here, :] = part

        each(0, piece // block, mix)

        def keep(r):
            group, offset = (r * 32) // TILE, (r * 32) % TILE
            kept = [mixed[pl.ds(picked(group, offset + u), 1), :] for u in range(32)]
            for u in range(0, 32, 8):
                y_out[c, pl.ds(pl.multiple_of(r * 32 + u, 8), 8), :] = jnp.concatenate(kept[u : u + 8], axis=0)

        each(0, room // 32, keep)
        each(1, far, lambda t: far_copy(c, t).start())
        y_got[c, span(b, share), :] = y_out[c, span(b, share), :]

    def last(c):
        each(1, far, lambda t: far_copy(c, t).wait_recv())
        lanes = pl.ds(pl.multiple_of(c * TILE, TILE), TILE)

        def mix(r):
            where = [pl.ds(pl.multiple_of(j * share + r * 16, 16), 16) for j in range(far)]
            for here, part in zip(where, butterfly([y_got[c, here, :] for here in where])):
                x_high, x_low = split(part * weights[here, :])
                high[here, lanes] = x_high
                low[here, lanes] = x_low

        each(0, share // 16, mix)

        def gram(i):
            left = pl.ds(pl.multiple_of(i * TILE, TILE), TILE)
            if groups:
                half = c // 2
                first = 2 * half * (half + 1) + (c % 2) * (2 * half + 2) + 2 * i - c
            else:
                half = i // 2
                first = 2 * steps * half - 2 * half * (half - 1) + (i % 2) * (steps - 2 * half)
            tile = dot3((high[:, left], low[:, left]), (high[:, lanes], low[:, lanes]), ((0,), (0,)))
            g_ref[span(first + c - i, TILE), :] = tile

        each(0, c + 1, gram)

    each(0, steps, lambda c: loading(c).start())
    barrier = pltpu.get_barrier_semaphore()

    def greet(there):
        pl.semaphore_signal(barrier, inc=1, device_id=there, device_id_type=MESH)

    each(1, near, lambda t: greet(at((a + t) % near, b)))
    each(1, far, lambda t: greet(at(a, (b + t) % far)))
    for i in range(rows // base):
        signed_h[i] = (h_ref[...] * s_ref[i : i + 1, :]).astype(jnp.bfloat16)
    sizes_list, starts = column_tiles(steps) if groups else panel_tiles(steps)
    for i in range(0 if groups else 1, steps, 2):
        spare = (starts[i] + sizes_list[i] - 1) * TILE
        g_ref[spare : spare + TILE, :] = jnp.zeros((TILE, TILE), jnp.float32)
    samples[me] = samples_ref[...]
    pl.semaphore_wait(barrier, near + far - 2)
    each(1, near, lambda t: sample_copy(t, 0).start())
    transform(0)
    each(1, near, lambda t: sample_copy(t, 0).wait_recv())
    each(1, far, lambda t: sample_copy(t, 1).start())
    each(1, ahead, transform)
    each(1, far, lambda t: sample_copy(t, 1).wait_recv())
    choose()

    if groups:
        pair, plane, line = groups

        def place(cc, qq, bb):
            return at(qq * pair + cc, bb)

        runs = list(zip(starts, sizes_list))
        stages, drain = reduce_stages(
            groups, (a % pair, a // pair, b, place), runs, g_ref, whole, in1, in2, in3, sum1, sum2, send, arrive
        )

    def stage_at(j, stage, delay):
        for k in range(steps - delay + 1 if groups else 0):
            pl.when(j == k + delay)(functools.partial(stages[stage], k))

    def step(c):
        stage_at(c, 1, 2)

        @pl.when(c + ahead < steps)
        def _():
            transform(c + ahead)

        @pl.when(c < steps)
        def _():
            middle(c)

        stage_at(c, 2, 3)

        @pl.when(c > 0)
        def _():
            last(c - 1)

        stage_at(c, 0, 1)
        stage_at(c, 3, 4)

    each(0, steps + 1, step)
    if groups:
        for wave in range(6):
            for k in reversed(range(steps)):
                stage = min(steps - k, 4) + wave
                if stage < len(stages):
                    stages[stage](k)
        over_ref[...] = whole[flag : flag + 8, :]
        for k, start in enumerate(starts):
            for i in range(k + 1):
                tile = (start + i) * TILE
                work[i * TILE : (i + 1) * TILE, k * TILE : (k + 1) * TILE] = whole[tile : tile + TILE, :]
        drain()
        share_rows = out_ref.shape[0]
        own = lax.axis_index("rows") * share_rows

        def keep_own(k, upper):
            row_block[...] = upper

            @pl.when(own // TILE == k)
            def _():
                out_ref[...] = row_block[pl.ds(pl.multiple_of(own % TILE, 8), share_rows), :]

        factor_panels(work, keep_own, spare_lines, row_high, row_low)
    each(1, near, lambda t: sample_copy(t, 0).wait_send())
    each(1, far, lambda t: sample_copy(t, 1).wait_send())
    each(0, steps, lambda c: each(1, near, lambda t: near_copy(c, t).wait_send()))
    each(0, steps, lambda c: each(1, far, lambda t: far_copy(c, t).wait_send()))


def exchange(matrix, row_signs, samples, near, far, room, scale, groups):
    rows, cols = matrix.shape
    steps = cols // TILE
    base = min(256, rows)
    lines = -(-samples.shape[0] // TILE)
    padded = jnp.pad(samples, (0, lines * TILE - samples.shape[0]), constant_values=-1).reshape(lines, TILE)
    tiles = sum(panel_tiles(steps)[0])
    vmem = pl.BlockSpec(memory_space=pltpu.VMEM)
    picks = -(-room // TILE)
    packed = tiles * TILE
    gram = jax.ShapeDtypeStruct((packed, TILE), jnp.float32)
    fused = []
    if groups:
        pair, plane, line = groups
        share_rows = cols // lax.axis_size("rows")
        outs = [jax.ShapeDtypeStruct((share_rows, cols), jnp.float32), jax.ShapeDtypeStruct((8, TILE), jnp.float32)]
        fused = [
            pltpu.VMEM((packed, TILE), jnp.float32),
            pltpu.VMEM((packed, TILE), jnp.float32),
            pltpu.VMEM((pair - 1, packed // pair, TILE), jnp.float32),
            pltpu.VMEM((plane - 1, packed // (pair * plane), TILE), jnp.float32),
            pltpu.VMEM((max(line - 1, 1), packed // (near * far), TILE), jnp.float32),
            pltpu.VMEM((packed // pair, TILE), jnp.float32),
            pltpu.VMEM((packed // (pair * plane), TILE), jnp.float32),
            pltpu.SemaphoreType.DMA((steps, 24)),
            pltpu.SemaphoreType.DMA((steps, 24)),
            pltpu.VMEM((cols, cols), jnp.float32),
            pltpu.VMEM((2, 10, 8, TILE), jnp.float32),
            pltpu.VMEM((TILE, cols), jnp.bfloat16),
            pltpu.VMEM((TILE, cols), jnp.bfloat16),
            pltpu.VMEM((TILE, cols), jnp.float32),
        ]
    return pl.pallas_call(
        functools.partial(exchange_kernel, (near, far, min(AHEAD, steps)), scale, groups),
        out_shape=outs if groups else gram,
        in_specs=[pl.BlockSpec(memory_space=pl.ANY), vmem, vmem, vmem],
        out_specs=[vmem, vmem] if groups else vmem,
        scratch_shapes=[
            pltpu.VMEM((steps, rows, TILE), jnp.float32),
            pltpu.VMEM((rows // base, base, base), jnp.bfloat16),
            pltpu.VMEM((steps, rows, TILE), jnp.float32),
            pltpu.VMEM((steps, rows, TILE), jnp.float32),
            pltpu.VMEM((rows, TILE), jnp.float32),
            pltpu.VMEM((steps, room, TILE), jnp.float32),
            pltpu.VMEM((steps, room, TILE), jnp.float32),
            pltpu.VMEM((room, cols), jnp.bfloat16),
            pltpu.VMEM((room, cols), jnp.bfloat16),
            pltpu.VMEM((near * far, lines, TILE), jnp.int32),
            pltpu.VMEM((far, rows, TILE), jnp.float32),
            pltpu.VMEM((room, TILE), jnp.float32),
            pltpu.VMEM((picks, TILE), jnp.int32),
            pltpu.SMEM((picks, TILE), jnp.int32),
            pltpu.SemaphoreType.DMA((steps + 1,)),
            pltpu.SemaphoreType.DMA((steps, near)),
            pltpu.SemaphoreType.DMA((steps, near)),
            pltpu.SemaphoreType.DMA((steps, far)),
            pltpu.SemaphoreType.DMA((steps, far)),
            pltpu.SemaphoreType.DMA((near + far,)),
            pltpu.SemaphoreType.DMA((near + far,)),
            *fused,
        ],
        compiler_params=pltpu.CompilerParams(vmem_limit_bytes=VMEM_LIMIT, collective_id=2, has_side_effects=True),
    )(matrix, row_signs.astype(jnp.float32).reshape(rows // base, base), sylvester(base), padded)


def whole_exchange(matrix, row_signs, all_indices, scale):
    blocks = lax.axis_size("rows") * lax.axis_size("grp")
    row_dev, col_count = matrix.shape
    piece_rows = row_dev // blocks
    position = lax.axis_index(("rows", "grp"))
    signs = jnp.broadcast_to(row_signs.astype(jnp.float32)[:, None], (row_dev, TILE))
    before = local_transform(matrix, signs, min(256, row_dev))
    arrived = lax.all_to_all(
        before.reshape(blocks, piece_rows, col_count),
        ("rows", "grp"),
        split_axis=0,
        concat_axis=0,
        tiled=True,
    )
    first = jnp.arange(blocks, dtype=jnp.int32)[:, None] * row_dev + position * piece_rows
    within = all_indices - first
    hits = within[:, None, :] == jnp.arange(piece_rows, dtype=jnp.int32)[None, :, None]
    weights = jnp.max(hits.astype(jnp.float32), axis=2)
    weights = jnp.broadcast_to(weights[:, :, None], (blocks, piece_rows, TILE))
    half = gram_share(arrived, weights, scale)
    whole = (half + half.T) * 0.5
    pieces = []
    for i, count in enumerate(panel_tiles(col_count // TILE)[0]):
        row = whole[i * TILE : (i + 1) * TILE]
        tiles = [row[:, j * TILE : (j + 1) * TILE] for j in range(i, col_count // TILE)]
        tiles += [jnp.zeros((TILE, TILE), jnp.float32)] * (count - len(tiles))
        pieces += tiles
    return jnp.concatenate(pieces, axis=0)


def shards(matrix, row_signs, samples):
    count_rows = lax.axis_size("rows")
    blocks = count_rows * lax.axis_size("grp")
    row_dev, col_count = matrix.shape
    sample_dev = samples.shape[0]
    scale = (sample_dev * blocks) ** -0.5
    far = 4
    near = blocks // far
    chance = 1.0 - (1.0 - sample_dev / row_dev) ** far
    room = row_dev * chance + 5.0 * (row_dev * chance * (1.0 - chance)) ** 0.5
    room = min(row_dev, -(-int(room) // (16 * far)) * 16 * far)
    share_rows = col_count // count_rows

    def own(upper_factor):
        return lax.dynamic_slice_in_dim(upper_factor, lax.axis_index("rows") * share_rows, share_rows, 0)

    groups = reduce_groups([tiles for tiles in column_tiles(col_count // TILE)[0]])
    if groups:
        mine, over = exchange(matrix, row_signs, samples, near, far, room, scale, groups)
    else:
        packed = exchange(matrix, row_signs, samples, near, far, room, scale, None)
        upper_factor, over = reduce_factor(packed, col_count)
        mine = own(upper_factor)

    def again():
        all_indices = lax.all_gather(samples, ("rows", "grp"), axis=0)
        packed = whole_exchange(matrix, row_signs, all_indices, scale)
        return own(reduce_factor(packed, col_count)[0])

    return lax.cond(over[0, 0] > 0.0, again, lambda: mine)


def solution(mesh):
    return jax.shard_map(
        shards,
        mesh=mesh,
        in_specs=(P(("rows", "grp"), None), P(("rows", "grp")), P(("rows", "grp"))),
        out_specs=P("rows", None),
        check_vma=False,
    )
```
